256 devices in a mesh: replica: 8 (over y, core), shard: 32 (over x, z).
Axes of the slice: x: 4, y: 4, z: 8, core: 2. Of those that a mesh axis runs over, the one named last changes fastest.
Arguments:
- deltas: bfloat16 [8, 64, 128, 6144], P('replica', None, 'shard')
- block_list: int32 [8, 64], replicated, may hold values from -1 to 127, as said below
- hosting: int32 [8, 16, 8], replicated, may hold values from 0 to 1, as said below
- counts: int32 [8, 128], replicated, may hold values from 1 to 63
- params: float32 [128, 128, 6144], P('shard', 'replica'), may hold values from -6 to 6
- momentum: float32 [128, 128, 6144], P('shard', 'replica'), may hold values from -4 to 4
Outputs:
- new_params: float32 [128, 128, 6144], P('shard', 'replica')
- new_momentum: float32 [128, 128, 6144], P('shard', 'replica')
- host_params: bfloat16 [8, 64, 128, 6144], P('replica', None, 'shard')
The draws below stay inside these ranges and needn't reach their ends.
Inputs may be any that keep to these rules, and one draw needn't show every extreme that they name: `block_list`: row r lists, each once and in any order, the blocks whose parameters replica r holds, with -1 in the other entries; block b is owned by shard b // 4, and at most 2 listed blocks of one row have the same owner. `hosting`: 1 only for blocks that appear in the replica's row of block_list.
All inputs are finite; a program needn't handle non-finite values.
Results may differ from the reference program's by a relative error of at most 0.001.
Values may be sent and summed in bfloat16 or wider, within the bound.
A program may use at most 128 MiB of HBM per device.

```python
import math
import jax
import jax.numpy as jnp
from jax import lax

D = 6144
EXPERTS = 8
LAYERS = 16
ROWS = 128
REPLICAS = 8
BLOCKS = 128
OWN = 4
CAP = 2
SLOTS = 64


def list_entries(key):
    base_key = jax.random.fold_in(key, 7)
    keys = jax.random.split(base_key, 6)
    shard_count = BLOCKS // OWN
    taken = jax.random.randint(keys[0], (REPLICAS, shard_count), 0, CAP + 1)
    forced = jax.random.randint(keys[1], (REPLICAS, 1), 0, shard_count)
    shared = jax.random.randint(keys[2], (), 0, shard_count)
    column = jnp.arange(shard_count)[None, :]
    taken = jnp.where((column == forced) | (column == shared), CAP, taken)
    popular = jax.random.randint(keys[3], (EXPERTS,), 0, 4)
    block_ids = jnp.arange(BLOCKS).reshape(shard_count, OWN)
    scores = jax.random.randint(keys[4], (REPLICAS, shard_count, OWN), 0, 1000)
    scores = (scores + 700 * popular[block_ids % EXPERTS][None]) * OWN + jnp.arange(OWN)
    order = jnp.argsort(-scores, axis=-1)
    chosen = jnp.take_along_axis(jnp.broadcast_to(block_ids[None], scores.shape), order, axis=-1)[:, :, :CAP]
    alive = jnp.arange(CAP)[None, None, :] < taken[:, :, None]
    entries = jnp.where(alive, chosen, -1).reshape(REPLICAS, SLOTS)
    shuffle = jax.random.randint(keys[5], (REPLICAS, SLOTS), 0, 1 << 20) * SLOTS + jnp.arange(SLOTS)
    return jnp.take_along_axis(entries, jnp.argsort(shuffle, axis=1), axis=1).astype(jnp.int32)


def draw_block_list(key, part):
    return list_entries(key)


def draw_hosting(key, part):
    entries = list_entries(key)
    member = jnp.any(entries[:, :, None] == jnp.arange(BLOCKS)[None, None, :], axis=1)
    coins = jax.random.randint(jax.random.fold_in(key, 8), (REPLICAS, BLOCKS), 0, 4)
    trained = jnp.where(member & (coins > 0), 1, 0)
    return trained.reshape(REPLICAS, LAYERS, EXPERTS).astype(jnp.int32)


def draw_deltas(key, part):
    entries = list_entries(key)
    noise_key, column_key = jax.random.split(jax.random.fold_in(key, 9))
    shape = (REPLICAS, SLOTS, ROWS, D)
    noise = jax.random.normal(noise_key, shape, jnp.float32)
    column_scale = jnp.exp(jax.random.uniform(column_key, (D,), jnp.float32, math.log(0.3), math.log(3.0)))
    row_scale = 10.0 ** (jnp.arange(ROWS).astype(jnp.float32) / max(ROWS - 1, 1))
    block_scale = 3.0 ** (jnp.maximum(entries, 0).astype(jnp.float32) / max(BLOCKS - 1, 1))
    values = 0.2 * noise * column_scale[None, None, None, :] * row_scale[None, None, :, None]
    values = values * block_scale[:, :, None, None]
    return values.astype(jnp.bfloat16)


def set_ends(drawn, rng, smallest, largest):
    extent = drawn.shape
    place = [jax.random.randint(jax.random.fold_in(rng, axis), (), 0, extent[axis]) for axis in range(len(extent))]
    drawn = drawn.at[tuple(place)].set(smallest)
    longest = extent.index(max(extent))
    place[longest] = (place[longest] + 1) % extent[longest]
    return drawn.at[tuple(place)].set(largest)


def block_levels(rng, dims, shards, smallest, high):
    def one(dim, parts):
        heights = jax.random.uniform(jax.random.fold_in(jax.random.fold_in(rng, 6), dim), (parts,), jnp.float32, smallest / len(shards), high / len(shards))
        return jnp.repeat(jnp.exp(heights), dims[dim] // parts).reshape((-1,) + (1,) * (len(dims) - dim - 1))

    factor_of = one(*shards[0])
    for cut in shards[1:]:
        factor_of = factor_of * one(*cut)
    return factor_of


def scatter_about(stream_key, dims, width, most, pieces=(), held_as=jnp.bfloat16):
    array = jax.random.normal(stream_key, dims, jnp.float32) * width
    if len(pieces) > 0:
        array = block_levels(stream_key, dims, pieces, -0.22, 0.18) * array
    return jnp.clip(array, min=-most, max=most).astype(held_as)


def setup_inputs(seed: int = 0) -> dict:
    seeds = jax.random.split(jax.random.key(seed), 7)
    deltas = draw_deltas(jax.random.fold_in(seeds[6], 71), 0)
    block_list = draw_block_list(jax.random.fold_in(seeds[6], 71), 0)
    hosting = draw_hosting(jax.random.fold_in(seeds[6], 71), 0)
    counts = set_ends(jax.random.randint(seeds[3], (REPLICAS, BLOCKS), 1, 64), jax.random.fold_in(seeds[3], 1), 1, 63).astype(jnp.int32)
    params = scatter_about(seeds[4], (BLOCKS, ROWS, D), 1.0, 6.0, ((0, 32), (1, 8)), jnp.float32)
    momentum = scatter_about(seeds[5], (BLOCKS, ROWS, D), 0.5, 4.0, ((0, 32), (1, 8)), jnp.float32)
    return dict(deltas=deltas, block_list=block_list, hosting=hosting, counts=counts, params=params, momentum=momentum)


def reference(deltas, block_list, hosting, counts, params, momentum):
    block_count = LAYERS * EXPERTS
    weight = hosting.reshape(REPLICAS, block_count) * counts
    totals = jnp.maximum(lax.optimization_barrier(jnp.sum(weight, axis=0)).astype(jnp.float32), 1.0)

    def add_replica(summed, members):
        rows_delta, listed, weight_row = members
        safe_index = jnp.where(listed >= 0, listed, 0).astype(jnp.int32)
        entry_weight = jnp.where(listed >= 0, weight_row[safe_index], 0).astype(jnp.float32)
        weighted = entry_weight[:, None, None] * rows_delta.astype(jnp.float32)
        return (summed.at[safe_index].add(weighted), None)
    start = jnp.zeros((block_count, ROWS, D), jnp.float32)
    summed, _ = lax.scan(add_replica, start, (deltas, block_list, weight))
    gradient = summed / totals[:, None, None]
    square_sum = jnp.sum(gradient * gradient)
    limit = 0.1 * math.sqrt(block_count * ROWS * D)
    clip_factor = jnp.minimum(1.0, limit / jnp.sqrt(square_sum + 1e-06))
    scaled = clip_factor * gradient
    new_momentum = 0.9 * momentum + scaled
    new_params = params - 0.7 * (scaled + 0.9 * new_momentum)
    hosted = new_params.astype(jnp.bfloat16)

    def pick_rows(listed):
        safe_index = jnp.where(listed >= 0, listed, 0).astype(jnp.int32)
        picked = hosted[safe_index]
        return jnp.where((listed >= 0)[:, None, None], picked, jnp.zeros_like(picked))
    host_params = lax.map(pick_rows, block_list)
    return (new_params, new_momentum, host_params)
```

```python
import functools
import math

import jax
import jax.numpy as jnp
from jax import lax
from jax.experimental import pallas as pl
from jax.experimental.pallas import tpu as pltpu
from jax.sharding import PartitionSpec as P

D = 6144
ROWS = 128
HALF = D // 2
CHUNKS = 4
DC = HALF // CHUNKS
SLOTS = 64
OWN = 4
CAP = 2
REPLICAS = 8
BLOCKS = 128
MESH = pl.DeviceIdType.MESH

decay_rate = 0.9
outer_rate = 0.7
limit_ratio = 0.1


class Place:
    def __init__(self):
        self.replica = lax.axis_index("replica")
        self.shard = lax.axis_index("shard")
        self.y = self.replica // 2
        self.c = self.replica % 2
        self.x = self.shard // 8
        self.z = self.shard % 8
        self.zh = self.z // 4
        self.zl = self.z % 4
        self.self_xy = self.x == self.y
        self.self_z = self.c == self.zh

    def xy_target(self, dx, dc):
        xt = lax.rem(self.x + dx, 4)
        ct = lax.rem(self.c + dc, 2)
        return xt, ct, (2 * self.x + ct, xt * 8 + self.z)

    def xy_source(self, d):
        r = lax.rem(self.replica + d, 8)
        return r, (r, self.y * 8 + self.z)

    def z_target(self, dz):
        zt = lax.rem(self.z + dz, 8)
        return zt, (2 * self.y + self.zh, self.x * 8 + zt)

    def z_source(self, d, dc):
        zs = lax.rem(self.zl + d, 4)
        cs = lax.rem(self.c + dc, 2)
        return zs, cs, (2 * self.y + cs, self.x * 8 + self.c * 4 + zs)

    def shifted(self, dx, dy, dz, dc):
        x = lax.rem(self.x + dx, 4)
        y = lax.rem(self.y + dy, 4)
        z = lax.rem(self.z + dz, 8)
        c = lax.rem(self.c + dc, 2)
        return (y * 2 + c, x * 8 + z)


def columns(half, n):
    return pl.ds(pl.multiple_of(half * HALF + n * DC, 128), DC)


def guarded(maybe_self, condition, act):
    if maybe_self:
        pl.when(jnp.logical_not(condition))(act)
    else:
        act()


def forward_kernel(
    index_ref, coef_ref, deltas_ref, grad_ref, square_ref,
    raw, packed, rx, sums, gx, sq_c, sq_x, sq_y, sq_z,
    load_sem, xy_send, xy_recv, z_send, z_recv, sq_send, sq_recv,
):
    me = Place()
    load = pltpu.make_async_copy(deltas_ref.at[0], raw, load_sem)
    load.start()

    barrier = pltpu.get_barrier_semaphore()

    def greet(device):
        pl.semaphore_signal(barrier, inc=1, device_id=device, device_id_type=MESH)

    for d in range(8):
        guarded(d == 0, me.self_xy, functools.partial(greet, me.xy_source(d)[1]))
    for d in range(4):
        for dc in range(2):
            guarded(d == 0 and dc == 0, me.self_z, functools.partial(greet, me.z_source(d, dc)[2]))
    stages = (
        (sq_c, me.c, [(0, 0, 0, 1)], lambda o: lax.rem(me.c + o[3], 2)),
        (sq_x, me.x, [(d, 0, 0, 0) for d in (1, 2, 3)], lambda o: lax.rem(me.x + o[0], 4)),
        (sq_y, me.y, [(0, d, 0, 0) for d in (1, 2, 3)], lambda o: lax.rem(me.y + o[1], 4)),
        (sq_z, me.z, [(0, 0, d, 0) for d in range(1, 8)], lambda o: lax.rem(me.z + o[2], 8)),
    )
    for _, _, offsets, _ in stages:
        for offset in offsets:
            greet(me.shifted(*offset))

    load.wait()

    def pack(p, carry):
        packed[p] = raw[index_ref[p]]
        return carry

    lax.fori_loop(0, SLOTS, pack, 0)

    pl.semaphore_wait(
        barrier,
        8 + 8 + 14 - me.self_xy.astype(jnp.int32) - me.self_z.astype(jnp.int32),
    )

    def xy_copy(n, dx, dc):
        xt, ct, device = me.xy_target(dx, dc)
        return pltpu.make_async_remote_copy(
            src_ref=packed.at[pl.ds(xt * 16, 16), :, columns(ct, n)],
            dst_ref=rx.at[n, me.replica],
            send_sem=xy_send.at[n, dx * 2 + dc],
            recv_sem=xy_recv.at[n, me.replica],
            device_id=device,
            device_id_type=MESH,
        )

    def xy_arrival(n, d):
        r, device = me.xy_source(d)
        return pltpu.make_async_remote_copy(
            src_ref=packed.at[pl.ds(0, 16), :, columns(0, n)],
            dst_ref=rx.at[n, r],
            send_sem=xy_send.at[n, 0],
            recv_sem=xy_recv.at[n, r],
            device_id=device,
            device_id_type=MESH,
        )

    def z_copy(n, dz):
        zt, device = me.z_target(dz)
        return pltpu.make_async_remote_copy(
            src_ref=sums.at[n, pl.ds(zt * 4, 4)],
            dst_ref=gx.at[n, me.zl * 2 + me.c],
            send_sem=z_send.at[n, dz],
            recv_sem=z_recv.at[n, me.zl * 2 + me.c],
            device_id=device,
            device_id_type=MESH,
        )

    def z_arrival(n, d, dc):
        zs, cs, device = me.z_source(d, dc)
        return pltpu.make_async_remote_copy(
            src_ref=sums.at[n, pl.ds(0, 4)],
            dst_ref=gx.at[n, zs * 2 + cs],
            send_sem=z_send.at[n, 0],
            recv_sem=z_recv.at[n, zs * 2 + cs],
            device_id=device,
            device_id_type=MESH,
        )

    xy_order = [(2, 0), (2, 1), (1, 0), (1, 1), (3, 0), (3, 1), (0, 1), (0, 0)]
    z_order = [4, 3, 5, 2, 6, 1, 7, 0]
    for n in range(CHUNKS):
        for dx, dc in xy_order:
            guarded(dx == 0 and dc == 0, me.self_xy, lambda n=n, dx=dx, dc=dc: xy_copy(n, dx, dc).start())

    @pl.when(me.self_xy)
    def _():
        for n in range(CHUNKS):

            def own(k, carry, n=n):
                rx[n, me.replica, k] = packed[me.x * 16 + k, :, columns(me.c, n)]
                return carry

            lax.fori_loop(0, 16, own, 0)

    total = jnp.zeros((4, DC), jnp.float32)
    for n in range(CHUNKS):
        for d in range(8):
            guarded(d == 0, me.self_xy, lambda n=n, d=d: xy_arrival(n, d).wait_recv())

        def mix(owner, total, n=n):
            acc = [jnp.zeros((4, DC), jnp.float32) for _ in range(OWN)]
            for r in range(REPLICAS):
                for k in range(CAP):
                    rows = rx[n, r, owner * CAP + k].astype(jnp.float32)
                    for j in range(OWN):
                        acc[j] = acc[j] + coef_ref[(r * 16 + owner * CAP + k) * OWN + j] * rows
            for j in range(OWN):
                sums[n, owner * OWN + j] = acc[j]
                total = total + acc[j] * acc[j]
            return total

        total = lax.fori_loop(0, 8, mix, total)
        for dz in z_order:
            guarded(dz == 0, me.self_z, lambda n=n, dz=dz: z_copy(n, dz).start())

        @pl.when(me.self_z)
        def _(n=n):
            for j in range(OWN):
                gx[n, me.zl * 2 + me.c, j] = sums[n, me.z * OWN + j]

    value = jnp.full((8, 128), jnp.sum(total), jnp.float32)
    first = 0
    for slots, mine, offsets, _ in stages:
        slots[mine] = value
        copies = []
        for i, offset in enumerate(offsets):
            copy = pltpu.make_async_remote_copy(
                src_ref=slots.at[mine],
                dst_ref=slots.at[mine],
                send_sem=sq_send.at[first + i],
                recv_sem=sq_recv.at[first + i],
                device_id=me.shifted(*offset),
                device_id_type=MESH,
            )
            copy.start()
            copies.append(copy)
        for copy in copies:
            copy.wait()
        value = slots[0]
        for i in range(1, slots.shape[0]):
            value = value + slots[i]
        first += len(offsets)
    square_ref[...] = value

    for n in range(CHUNKS):
        for d in range(4):
            for dc in range(2):
                guarded(
                    d == 0 and dc == 0, me.self_z, lambda n=n, d=d, dc=dc: z_arrival(n, d, dc).wait_recv()
                )
        for half in range(2):
            for pair in range(2):
                for j in range(OWN):
                    grad_ref[j, pair * 8 : pair * 8 + 8, half * HALF + n * DC : half * HALF + n * DC + DC] = (
                        jnp.concatenate([gx[n, pair * 4 + half, j], gx[n, pair * 4 + 2 + half, j]], axis=0)
                    )

    for n in range(CHUNKS):
        for dx, dc in xy_order:
            guarded(dx == 0 and dc == 0, me.self_xy, lambda n=n, dx=dx, dc=dc: xy_copy(n, dx, dc).wait_send())
        for dz in z_order:
            guarded(dz == 0, me.self_z, lambda n=n, dz=dz: z_copy(n, dz).wait_send())


def forward(index, coef, deltas):
    vmem, dma = pltpu.VMEM, pltpu.SemaphoreType.DMA
    return pl.pallas_call(
        forward_kernel,
        out_shape=(
            jax.ShapeDtypeStruct((OWN, 16, D), jnp.float32),
            jax.ShapeDtypeStruct((8, 128), jnp.float32),
        ),
        in_specs=[
            pl.BlockSpec(memory_space=pltpu.SMEM),
            pl.BlockSpec(memory_space=pltpu.SMEM),
            pl.BlockSpec(memory_space=pl.ANY),
        ],
        out_specs=(pl.BlockSpec(memory_space=vmem), pl.BlockSpec(memory_space=vmem)),
        scratch_shapes=[
            vmem((SLOTS, 4, D), jnp.bfloat16),
            vmem((SLOTS, 4, D), jnp.bfloat16),
            vmem((CHUNKS, REPLICAS, 16, 4, DC), jnp.bfloat16),
            vmem((CHUNKS, 32, 4, DC), jnp.float32),
            vmem((CHUNKS, 8, OWN, 4, DC), jnp.float32),
            vmem((2, 8, 128), jnp.float32),
            vmem((4, 8, 128), jnp.float32),
            vmem((4, 8, 128), jnp.float32),
            vmem((8, 8, 128), jnp.float32),
            dma,
            dma((CHUNKS, 8)),
            dma((CHUNKS, 8)),
            dma((CHUNKS, 8)),
            dma((CHUNKS, 8)),
            dma((14,)),
            dma((14,)),
        ],
        compiler_params=pltpu.CompilerParams(
            collective_id=0, has_side_effects=True, vmem_limit_bytes=40 * 2**20
        ),
        name="forward_exchange",
    )(index, coef, deltas)


def update_kernel(square_ref, grad_ref, params_ref, momentum_ref, new_params_ref, new_momentum_ref, hosted_ref):
    limit = limit_ratio * math.sqrt(BLOCKS * ROWS * D)
    square = square_ref[0:1, 0:1]
    factor = jnp.minimum(1.0, limit / jnp.sqrt(square + 1e-06))
    for j in range(OWN):
        for pair in range(2):
            rows = slice(pair * 8, pair * 8 + 8)
            scaled = factor * grad_ref[j, rows, :]
            new_momentum = decay_rate * momentum_ref[j, rows, :] + scaled
            new_params = params_ref[j, rows, :] - outer_rate * (scaled + decay_rate * new_momentum)
            new_momentum_ref[j, rows, :] = new_momentum
            new_params_ref[j, rows, :] = new_params
            hosted = new_params.astype(jnp.bfloat16)
            hosted_ref[pair * 2, j] = hosted[0:4]
            hosted_ref[pair * 2 + 1, j] = hosted[4:8]


def update(square, grad, params, momentum):
    width = 1024
    wide = pl.BlockSpec((OWN, 16, width), lambda i: (0, 0, i))
    return pl.pallas_call(
        update_kernel,
        grid=(D // width,),
        out_shape=(
            jax.ShapeDtypeStruct((OWN, 16, D), jnp.float32),
            jax.ShapeDtypeStruct((OWN, 16, D), jnp.float32),
            jax.ShapeDtypeStruct((4, OWN, 4, D), jnp.bfloat16),
        ),
        in_specs=[pl.BlockSpec((8, 128), lambda i: (0, 0)), wide, wide, wide],
        out_specs=(wide, wide, pl.BlockSpec((4, OWN, 4, width), lambda i: (0, 0, 0, i))),
        compiler_params=pltpu.CompilerParams(vmem_limit_bytes=40 * 2**20),
        name="outer_update",
    )(square, grad, params, momentum)


def return_kernel(list_ref, hosted_ref, out_ref, *scratch):
    gathered = scratch[0]
    near = scratch[1 : 1 + CHUNKS]
    far = scratch[1 + CHUNKS : 1 + 2 * CHUNKS]
    z_send, z_recv, y_send, y_recv, x_send, x_recv, d_send, d_recv = scratch[1 + 2 * CHUNKS :]
    me = Place()
    sibling = (2 * me.y + 1 - me.c, me.shard)

    barrier = pltpu.get_barrier_semaphore()

    def greet(device):
        pl.semaphore_signal(barrier, inc=1, device_id=device, device_id_type=MESH)

    def z_target(d, dc):
        return me.z_source(d, dc)

    def z_source(dz):
        return me.z_target(dz)

    for dz in range(8):
        guarded(dz == 0, me.self_z, functools.partial(greet, z_source(dz)[1]))
    for d in (1, 2, 3):
        greet(me.shifted(0, d, 0, 0))
        greet(me.shifted(d, 0, 0, 0))
    greet(sibling)
    pl.semaphore_wait(barrier, 8 + 6 + 1 - me.self_z.astype(jnp.int32))

    def z_copy(n, d, dc):
        zt, ct, device = z_target(d, dc)
        return pltpu.make_async_remote_copy(
            src_ref=hosted_ref.at[zt, :, :, columns(ct, n)],
            dst_ref=gathered.at[n, me.y, me.z],
            send_sem=z_send.at[n, d * 2 + dc],
            recv_sem=z_recv.at[n, me.z],
            device_id=device,
            device_id_type=MESH,
        )

    def z_arrival(n, dz):
        zs, device = z_source(dz)
        return pltpu.make_async_remote_copy(
            src_ref=hosted_ref.at[0, :, :, columns(0, n)],
            dst_ref=gathered.at[n, me.y, zs],
            send_sem=z_send.at[n, 0],
            recv_sem=z_recv.at[n, zs],
            device_id=device,
            device_id_type=MESH,
        )

    def y_copy(n, d, arrival=False):
        ys = lax.rem(me.y + d, 4) if arrival else me.y
        return pltpu.make_async_remote_copy(
            src_ref=gathered.at[n, ys],
            dst_ref=gathered.at[n, ys],
            send_sem=y_send.at[n, d],
            recv_sem=y_recv.at[n, ys],
            device_id=me.shifted(0, d, 0, 0),
            device_id_type=MESH,
        )

    def x_copy(n, d):
        return pltpu.make_async_remote_copy(
            src_ref=gathered.at[n, lax.rem(me.x + d, 4)],
            dst_ref=near[n].at[me.x],
            send_sem=x_send.at[n, d],
            recv_sem=x_recv.at[n, me.x],
            device_id=me.shifted(d, 0, 0, 0),
            device_id_type=MESH,
        )

    def x_arrival(n, d):
        xs = lax.rem(me.x + d, 4)
        return pltpu.make_async_remote_copy(
            src_ref=gathered.at[n, xs],
            dst_ref=near[n].at[xs],
            send_sem=x_send.at[n, d],
            recv_sem=x_recv.at[n, xs],
            device_id=me.shifted(d, 0, 0, 0),
            device_id_type=MESH,
        )

    def d_copy(n, d):
        xs = lax.rem(me.x + d, 4)
        return pltpu.make_async_remote_copy(
            src_ref=near[n].at[xs],
            dst_ref=far[n].at[xs],
            send_sem=d_send.at[n, xs],
            recv_sem=d_recv.at[n, xs],
            device_id=sibling,
            device_id_type=MESH,
        )

    z_order = [(d, dc) for d in (2, 1, 3, 0) for dc in (0, 1)]
    order = (2, 1, 3)

    def start_z(n):
        for d, dc in z_order:
            guarded(d == 0 and dc == 0, me.self_z, lambda d=d, dc=dc: z_copy(n, d, dc).start())

        @pl.when(me.self_z)
        def _():
            for j in range(OWN):
                gathered[n, me.y, me.z, j] = hosted_ref[me.zl, j, :, columns(me.c, n)]

    def start_y(n):
        for dz in range(8):
            guarded(dz == 0, me.self_z, lambda dz=dz: z_arrival(n, dz).wait_recv())
        for d in order:
            y_copy(n, d).start()

    def start_x(n):
        for d in order:
            y_copy(n, d, arrival=True).wait_recv()
        for d in order:
            x_copy(n, d).start()

        def own(owner, carry):
            for j in range(OWN):
                near[n][me.x, owner, j] = gathered[n, me.x, owner, j]
            return carry

        lax.fori_loop(0, 8, own, 0)

    def start_d(n):
        d_copy(n, 0).start()
        for d in order:
            x_arrival(n, d).wait_recv()
            d_copy(n, d).start()

    def unpack(n):
        for d in range(4):
            d_copy(n, d).wait_recv()

        def entry(k, carry):
            block = list_ref[me.replica * SLOTS + k]
            safe = jnp.maximum(block, 0)
            for rows, half in ((near[n], me.c), (far[n], 1 - me.c)):
                value = rows[safe // 32, (safe // 4) % 8, safe % 4]
                out_ref[0, k, :, columns(half, n)] = jnp.where(block >= 0, value, jnp.zeros_like(value))
            return carry

        lax.fori_loop(0, SLOTS, entry, 0)

    for n in range(CHUNKS):
        start_z(n)
    for step in range(CHUNKS + 3):
        for lag, stage in enumerate((start_y, start_x, start_d, unpack)):
            if 0 <= step - lag < CHUNKS:
                stage(step - lag)

    for n in range(CHUNKS):
        for d, dc in z_order:
            guarded(d == 0 and dc == 0, me.self_z, lambda n=n, d=d, dc=dc: z_copy(n, d, dc).wait_send())
        for d in order:
            y_copy(n, d).wait_send()
            x_copy(n, d).wait_send()
        for d in range(4):
            d_copy(n, d).wait_send()


def send_back(lists, hosted):
    vmem, dma = pltpu.VMEM, pltpu.SemaphoreType.DMA
    return pl.pallas_call(
        return_kernel,
        out_shape=jax.ShapeDtypeStruct((1, SLOTS, 4, D), jnp.bfloat16),
        in_specs=[pl.BlockSpec(memory_space=pltpu.SMEM), pl.BlockSpec(memory_space=vmem)],
        out_specs=pl.BlockSpec(memory_space=vmem),
        scratch_shapes=[vmem((CHUNKS, 4, 8, OWN, 4, DC), jnp.bfloat16)]
        + [vmem((4, 8, OWN, 4, DC), jnp.bfloat16)] * (2 * CHUNKS)
        + [
            dma((CHUNKS, 8)),
            dma((CHUNKS, 8)),
            dma((CHUNKS, 4)),
            dma((CHUNKS, 4)),
            dma((CHUNKS, 4)),
            dma((CHUNKS, 4)),
            dma((CHUNKS, 4)),
            dma((CHUNKS, 4)),
        ],
        compiler_params=pltpu.CompilerParams(
            collective_id=1, has_side_effects=True, vmem_limit_bytes=40 * 2**20
        ),
        name="return_exchange",
    )(lists, hosted)


def tables(block_list, hosting, counts):
    x = lax.axis_index("shard") // 8
    weight = hosting.reshape(REPLICAS, BLOCKS) * counts
    totals = jnp.maximum(jnp.sum(weight, axis=0).astype(jnp.float32), 1.0)
    ratio = weight.astype(jnp.float32) / totals
    listed = block_list >= 0
    owner = jnp.where(listed, block_list // OWN, -1)
    earlier = jnp.arange(SLOTS)[:, None] < jnp.arange(SLOTS)[None, :]
    same = (owner[:, :, None] == owner[:, None, :]) & earlier[None]
    rank = jnp.sum(same.astype(jnp.int32), axis=1)
    place = jnp.where(listed, owner * CAP + rank, -1)
    my_place = lax.dynamic_index_in_dim(place, lax.axis_index("replica"), 0, keepdims=False)
    found = my_place[None, :] == jnp.arange(SLOTS)[:, None]
    index = jnp.sum(jnp.where(found, jnp.arange(SLOTS)[None, :], 0), axis=1)
    wanted = x * 16 + jnp.arange(16)
    block = jnp.sum(jnp.where(place[:, None, :] == wanted[None, :, None], block_list[:, None, :] + 1, 0), axis=2) - 1
    mine = lax.dynamic_slice_in_dim(ratio, x * 32, 32, 1).reshape(REPLICAS, 8, 1, OWN)
    target = (x * 32 + jnp.arange(32)).reshape(1, 8, 1, OWN)
    coef = jnp.where(block.reshape(REPLICAS, 8, CAP, 1) == target, mine, 0.0)
    return index.astype(jnp.int32), coef.reshape(-1)


def per_device(deltas, block_list, hosting, counts, params, momentum):
    index, coef = tables(block_list, hosting, counts)
    grad, square = forward(index, coef, deltas)
    new_params, new_momentum, hosted = update(square, grad, params, momentum)
    host_params = send_back(block_list.reshape(-1), hosted)
    return new_params, new_momentum, host_params


def solution(mesh):
    blocks = P("shard", "replica", None)
    entries = P("replica", None, "shard", None)
    return jax.shard_map(
        per_device,
        mesh=mesh,
        in_specs=(entries, P(), P(), P(), blocks, blocks),
        out_specs=(blocks, blocks, entries),
        check_vma=False,
    )
```

```python
import functools
import math

import jax
import jax.numpy as jnp
from jax import lax
from jax.experimental import pallas as pl
from jax.experimental.pallas import tpu as pltpu
from jax.sharding import PartitionSpec as P

D = 6144
ROWS = 128
HALF = D // 2
CHUNKS = 8
DC = HALF // CHUNKS
SLOTS = 64
OWN = 4
CAP = 2
REPLICAS = 8
BLOCKS = 128
MESH = pl.DeviceIdType.MESH

decay_rate = 0.9
outer_rate = 0.7
limit_ratio = 0.1


class Place:
    def __init__(self):
        self.replica = lax.axis_index("replica")
        self.shard = lax.axis_index("shard")
        self.y = self.replica // 2
        self.c = self.replica % 2
        self.x = self.shard // 8
        self.z = self.shard % 8
        self.zh = self.z // 4
        self.zl = self.z % 4
        self.self_xy = self.x == self.y
        self.self_z = self.c == self.zh

    def xy_target(self, dx, dc):
        xt = lax.rem(self.x + dx, 4)
        ct = lax.rem(self.c + dc, 2)
        return xt, ct, (2 * self.x + ct, xt * 8 + self.z)

    def xy_source(self, d):
        r = lax.rem(self.replica + d, 8)
        return r, (r, self.y * 8 + self.z)

    def z_target(self, dz):
        zt = lax.rem(self.z + dz, 8)
        return zt, (2 * self.y + self.zh, self.x * 8 + zt)

    def z_source(self, d, dc):
        zs = lax.rem(self.zl + d, 4)
        cs = lax.rem(self.c + dc, 2)
        return zs, cs, (2 * self.y + cs, self.x * 8 + self.c * 4 + zs)

    def shifted(self, dx, dy, dz, dc):
        x = lax.rem(self.x + dx, 4)
        y = lax.rem(self.y + dy, 4)
        z = lax.rem(self.z + dz, 8)
        c = lax.rem(self.c + dc, 2)
        return (y * 2 + c, x * 8 + z)


def columns(half, n):
    return pl.ds(pl.multiple_of(half * HALF + n * DC, 128), DC)


def guarded(maybe_self, condition, act):
    if maybe_self:
        pl.when(jnp.logical_not(condition))(act)
    else:
        act()


def exchange_kernel(
    capacity, table_ref, coef_ref, deltas_ref, params_ref, momentum_ref,
    new_params_ref, new_momentum_ref, host_ref, *scratch,
):
    (
        raw, packed, rx, sums, gx, sq_c, sq_x, sq_y, sq_z, params, momentum, new_params, new_momentum,
        hosted, picked, relay, host,
    ) = scratch[:17]
    blocks = scratch[17 : 17 + CHUNKS]
    near = scratch[17 + CHUNKS : 17 + 2 * CHUNKS]
    far = scratch[17 + 2 * CHUNKS : 17 + 3 * CHUNKS]
    (
        load_sem, xy_send, xy_recv, z_send, z_recv, sq_send, sq_recv,
        b_send, b_recv, y_send, y_recv, x_send, x_recv, d_send, d_recv, host_sem,
    ) = scratch[17 + 3 * CHUNKS :]
    me = Place()
    sibling = (2 * me.y + 1 - me.c, me.shard)
    load = pltpu.make_async_copy(deltas_ref.at[0], raw, load_sem.at[0])
    load.start()
    load_params = pltpu.make_async_copy(params_ref, params, load_sem.at[1])
    load_momentum = pltpu.make_async_copy(momentum_ref, momentum, load_sem.at[2])
    load_params.start()
    load_momentum.start()

    barrier = pltpu.get_barrier_semaphore()

    def greet(device):
        pl.semaphore_signal(barrier, inc=1, device_id=device, device_id_type=MESH)

    for d in range(8):
        guarded(d == 0, me.self_xy, functools.partial(greet, me.xy_source(d)[1]))
        guarded(d == 0, me.self_z, functools.partial(greet, me.z_target(d)[1]))
    for d in range(4):
        for dc in range(2):
            guarded(d == 0 and dc == 0, me.self_z, functools.partial(greet, me.z_source(d, dc)[2]))
    stages = (
        (sq_c, me.c, [(0, 0, 0, 1)]),
        (sq_x, me.x, [(d, 0, 0, 0) for d in (1, 2, 3)]),
        (sq_y, me.y, [(0, d, 0, 0) for d in (1, 2, 3)]),
        (sq_z, me.z, [(0, 0, d, 0) for d in range(1, 8)]),
    )
    for _, _, offsets in stages:
        for offset in offsets:
            greet(me.shifted(*offset))

    load.wait()

    def pack(owner, carry):
        for k in range(CAP):
            packed[owner * CAP + k] = raw[table_ref[k, owner]]
        return carry

    lax.fori_loop(0, 32, pack, 0)

    pl.semaphore_wait(
        barrier,
        8 + 16 + 14 - me.self_xy.astype(jnp.int32) - 2 * me.self_z.astype(jnp.int32),
    )

    def xy_copy(n, dx, dc):
        xt, ct, device = me.xy_target(dx, dc)
        return pltpu.make_async_remote_copy(
            src_ref=packed.at[pl.ds(xt * 16, 16), :, columns(ct, n)],
            dst_ref=rx.at[n, me.replica],
            send_sem=xy_send.at[n, dx * 2 + dc],
            recv_sem=xy_recv.at[n, me.replica],
            device_id=device,
            device_id_type=MESH,
        )

    def xy_arrival(n, d):
        r, device = me.xy_source(d)
        return pltpu.make_async_remote_copy(
            src_ref=packed.at[pl.ds(0, 16), :, columns(0, n)],
            dst_ref=rx.at[n, r],
            send_sem=xy_send.at[n, 0],
            recv_sem=xy_recv.at[n, r],
            device_id=device,
            device_id_type=MESH,
        )

    def z_copy(n, dz):
        zt, device = me.z_target(dz)
        return pltpu.make_async_remote_copy(
            src_ref=sums.at[n, pl.ds(zt * 4, 4)],
            dst_ref=gx.at[n, me.zl * 2 + me.c],
            send_sem=z_send.at[n, dz],
            recv_sem=z_recv.at[n, me.zl * 2 + me.c],
            device_id=device,
            device_id_type=MESH,
        )

    def z_arrival(n, d, dc):
        zs, cs, device = me.z_source(d, dc)
        return pltpu.make_async_remote_copy(
            src_ref=sums.at[n, pl.ds(0, 4)],
            dst_ref=gx.at[n, zs * 2 + cs],
            send_sem=z_send.at[n, 0],
            recv_sem=z_recv.at[n, zs * 2 + cs],
            device_id=device,
            device_id_type=MESH,
        )

    xy_order = [(2, 0), (2, 1), (1, 0), (1, 1), (3, 0), (3, 1), (0, 1), (0, 0)]
    z_order = [4, 3, 5, 2, 6, 1, 7, 0]
    for n in range(CHUNKS):
        for dx, dc in xy_order:
            guarded(dx == 0 and dc == 0, me.self_xy, lambda n=n, dx=dx, dc=dc: xy_copy(n, dx, dc).start())

    @pl.when(me.self_xy)
    def _():
        for n in range(CHUNKS):

            def own(k, carry, n=n):
                rx[n, me.replica, k] = packed[me.x * 16 + k, :, columns(me.c, n)]
                return carry

            lax.fori_loop(0, 16, own, 0)

    total = jnp.zeros((4, DC), jnp.float32)
    for n in range(CHUNKS):
        for d in range(8):
            guarded(d == 0, me.self_xy, lambda n=n, d=d: xy_arrival(n, d).wait_recv())

        def mix(owner, total, n=n):
            acc = [jnp.zeros((4, DC), jnp.float32) for _ in range(OWN)]
            for r in range(REPLICAS):
                for k in range(CAP):
                    rows = rx[n, r, owner * CAP + k].astype(jnp.float32)
                    for j in range(OWN):
                        acc[j] = acc[j] + coef_ref[k * REPLICAS + r, me.x * 32 + owner * OWN + j] * rows
            for j in range(OWN):
                sums[n, owner * OWN + j] = acc[j]
                total = total + acc[j] * acc[j]
            return total

        total = lax.fori_loop(0, 8, mix, total)
        for dz in z_order:
            guarded(dz == 0, me.self_z, lambda n=n, dz=dz: z_copy(n, dz).start())

        @pl.when(me.self_z)
        def _(n=n):
            for j in range(OWN):
                gx[n, me.zl * 2 + me.c, j] = sums[n, me.z * OWN + j]

    value = jnp.full((8, 128), jnp.sum(total), jnp.float32)
    first = 0
    for slots, mine, offsets in stages:
        slots[mine] = value
        copies = []
        for i, offset in enumerate(offsets):
            copy = pltpu.make_async_remote_copy(
                src_ref=slots.at[mine],
                dst_ref=slots.at[mine],
                send_sem=sq_send.at[first + i],
                recv_sem=sq_recv.at[first + i],
                device_id=me.shifted(*offset),
                device_id_type=MESH,
            )
            copy.start()
            copies.append(copy)
        for copy in copies:
            copy.wait()
        value = slots[0]
        for i in range(1, slots.shape[0]):
            value = value + slots[i]
        first += len(offsets)

    def b_copy(n, d, dc):
        zt, ct, device = me.z_source(d, dc)
        return pltpu.make_async_remote_copy(
            src_ref=hosted.at[n, ct, zt],
            dst_ref=blocks[n].at[pl.ds(me.z * OWN, OWN)],
            send_sem=b_send.at[n, d * 2 + dc],
            recv_sem=b_recv.at[n, me.z],
            device_id=device,
            device_id_type=MESH,
        )

    def b_arrival(n, dz):
        zs, device = me.z_target(dz)
        return pltpu.make_async_remote_copy(
            src_ref=hosted.at[n, 0, 0],
            dst_ref=blocks[n].at[pl.ds(zs * OWN, OWN)],
            send_sem=b_send.at[n, 0],
            recv_sem=b_recv.at[n, zs],
            device_id=device,
            device_id_type=MESH,
        )

    b_order = [(d, dc) for d in (2, 1, 3, 0) for dc in (0, 1)]
    limit = limit_ratio * math.sqrt(BLOCKS * ROWS * D)
    factor = jnp.minimum(1.0, limit / jnp.sqrt(value + 1e-06))[0:1, 0:1]
    load_params.wait()
    load_momentum.wait()
    for n in range(CHUNKS):
        for d in range(4):
            for dc in range(2):
                guarded(
                    d == 0 and dc == 0, me.self_z, lambda n=n, d=d, dc=dc: z_arrival(n, d, dc).wait_recv()
                )
        for half in range(2):
            wide = slice(half * HALF + n * DC, half * HALF + n * DC + DC)
            for pair in range(2):
                rows = slice(pair * 8, pair * 8 + 8)
                for j in range(OWN):
                    grad = jnp.concatenate([gx[n, pair * 4 + half, j], gx[n, pair * 4 + 2 + half, j]], axis=0)
                    scaled = factor * grad
                    moved = decay_rate * momentum[j, rows, wide] + scaled
                    fresh = params[j, rows, wide] - outer_rate * (scaled + decay_rate * moved)
                    new_momentum[j, rows, wide] = moved
                    new_params[j, rows, wide] = fresh
                    rounded = fresh.astype(jnp.bfloat16)
                    hosted[n, half, pair * 2, j] = rounded[0:4]
                    hosted[n, half, pair * 2 + 1, j] = rounded[4:8]
        for d, dc in b_order:
            guarded(d == 0 and dc == 0, me.self_z, lambda n=n, d=d, dc=dc: b_copy(n, d, dc).start())

        @pl.when(me.self_z)
        def _(n=n):
            for j in range(OWN):
                blocks[n][me.z * OWN + j] = hosted[n, me.c, me.zl, j]

    store_params = pltpu.make_async_copy(new_params, new_params_ref, load_sem.at[1])
    store_momentum = pltpu.make_async_copy(new_momentum, new_momentum_ref, load_sem.at[2])
    store_params.start()
    store_momentum.start()

    def y_copy(n, d, arrival=False):
        ys = lax.rem(me.y + d, 4) if arrival else me.y
        return pltpu.make_async_remote_copy(
            src_ref=picked.at[n, d - 1],
            dst_ref=relay.at[n, ys],
            send_sem=y_send.at[n, d],
            recv_sem=y_recv.at[n, ys],
            device_id=me.shifted(0, d, 0, 0),
            device_id_type=MESH,
        )

    def x_copy(n, d, arrival=False):
        xs = lax.rem(me.x + d, 4)
        xd = xs if arrival else me.x
        return pltpu.make_async_remote_copy(
            src_ref=relay.at[n, xs],
            dst_ref=near[n].at[pl.ds(xd * capacity, capacity)],
            send_sem=x_send.at[n, d],
            recv_sem=x_recv.at[n, xd],
            device_id=me.shifted(d, 0, 0, 0),
            device_id_type=MESH,
        )

    def d_copy(n, d):
        xs = lax.rem(me.x + d, 4)
        return pltpu.make_async_remote_copy(
            src_ref=near[n].at[pl.ds(xs * capacity, capacity)],
            dst_ref=far[n].at[pl.ds(xs * capacity, capacity)],
            send_sem=d_send.at[n, xs],
            recv_sem=d_recv.at[n, xs],
            device_id=sibling,
            device_id_type=MESH,
        )

    def host_copy(n, half):
        return pltpu.make_async_copy(
            host.at[:, :, columns(half, n)], host_ref.at[0, :, :, columns(half, n)], host_sem.at[n, half]
        )

    order = (2, 1, 3)

    def start_y(n):
        for dz in range(8):
            guarded(dz == 0, me.self_z, lambda dz=dz: b_arrival(n, dz).wait_recv())

        def pick(k, carry):
            for d in range(1, 4):
                picked[n, d - 1, k] = blocks[n][table_ref[8 + lax.rem(me.y + d, 4) * 4 + me.x, k]]
            relay[n, me.y, k] = blocks[n][table_ref[8 + me.y * 4 + me.x, k]]
            return carry

        lax.fori_loop(0, capacity, pick, 0)
        for d in order:
            y_copy(n, d).start()

    def start_x(n):
        for d in order:
            y_copy(n, d, arrival=True).wait_recv()
        for d in order:
            x_copy(n, d).start()

        def own(k, carry):
            near[n][me.x * capacity + k] = relay[n, me.x, k]
            return carry

        lax.fori_loop(0, capacity, own, 0)

    def start_d(n):
        d_copy(n, 0).start()
        for d in order:
            x_copy(n, d, arrival=True).wait_recv()
            d_copy(n, d).start()

    def unpack(n):
        for d in range(4):
            d_copy(n, d).wait_recv()

        def entry(k, carry):
            place = table_ref[2, k]
            safe = table_ref[3, k] * capacity + jnp.maximum(place, 0)
            for rows, half in ((near[n], me.c), (far[n], 1 - me.c)):
                value = rows[safe]
                host[k, :, columns(half, n)] = jnp.where(place >= 0, value, jnp.zeros_like(value))
            return carry

        lax.fori_loop(0, SLOTS, entry, 0)
        for half in range(2):
            host_copy(n, half).start()

    for step in range(CHUNKS + 3):
        for lag, stage in enumerate((start_y, start_x, start_d, unpack)):
            if 0 <= step - lag < CHUNKS:
                stage(step - lag)

    for n in range(CHUNKS):
        for dx, dc in xy_order:
            guarded(dx == 0 and dc == 0, me.self_xy, lambda n=n, dx=dx, dc=dc: xy_copy(n, dx, dc).wait_send())
        for dz in z_order:
            guarded(dz == 0, me.self_z, lambda n=n, dz=dz: z_copy(n, dz).wait_send())
        for d, dc in b_order:
            guarded(d == 0 and dc == 0, me.self_z, lambda n=n, d=d, dc=dc: b_copy(n, d, dc).wait_send())
        for d in order:
            y_copy(n, d).wait_send()
            x_copy(n, d).wait_send()
        for d in range(4):
            d_copy(n, d).wait_send()
    store_params.wait()
    store_momentum.wait()
    for n in range(CHUNKS):
        for half in range(2):
            host_copy(n, half).wait()


def exchange(capacity, table, coef, deltas, params, momentum):
    vmem, dma = pltpu.VMEM, pltpu.SemaphoreType.DMA
    smem, anywhere = pl.BlockSpec(memory_space=pltpu.SMEM), pl.BlockSpec(memory_space=pl.ANY)
    owned = jax.ShapeDtypeStruct((OWN, 16, D), jnp.float32)
    return pl.pallas_call(
        functools.partial(exchange_kernel, capacity),
        out_shape=(owned, owned, jax.ShapeDtypeStruct((1, SLOTS, 4, D), jnp.bfloat16)),
        in_specs=[smem, smem, anywhere, anywhere, anywhere],
        out_specs=(anywhere, anywhere, anywhere),
        scratch_shapes=[
            vmem((SLOTS, 4, D), jnp.bfloat16),
            vmem((SLOTS, 4, D), jnp.bfloat16),
            vmem((CHUNKS, REPLICAS, 16, 4, DC), jnp.bfloat16),
            vmem((CHUNKS, 32, 4, DC), jnp.float32),
            vmem((CHUNKS, 8, OWN, 4, DC), jnp.float32),
            vmem((2, 8, 128), jnp.float32),
            vmem((4, 8, 128), jnp.float32),
            vmem((4, 8, 128), jnp.float32),
            vmem((8, 8, 128), jnp.float32),
            vmem((OWN, 16, D), jnp.float32),
            vmem((OWN, 16, D), jnp.float32),
            vmem((OWN, 16, D), jnp.float32),
            vmem((OWN, 16, D), jnp.float32),
            vmem((CHUNKS, 2, 4, OWN, 4, DC), jnp.bfloat16),
            vmem((CHUNKS, 3, capacity, 4, DC), jnp.bfloat16),
            vmem((CHUNKS, 4, capacity, 4, DC), jnp.bfloat16),
            vmem((SLOTS, 4, D), jnp.bfloat16),
        ]
        + [vmem((32, 4, DC), jnp.bfloat16)] * CHUNKS
        + [vmem((4 * capacity, 4, DC), jnp.bfloat16)] * (2 * CHUNKS)
        + [
            dma((3,)),
            dma((CHUNKS, 8)),
            dma((CHUNKS, 8)),
            dma((CHUNKS, 8)),
            dma((CHUNKS, 8)),
            dma((14,)),
            dma((14,)),
            dma((CHUNKS, 8)),
            dma((CHUNKS, 8)),
            dma((CHUNKS, 4)),
            dma((CHUNKS, 4)),
            dma((CHUNKS, 4)),
            dma((CHUNKS, 4)),
            dma((CHUNKS, 4)),
            dma((CHUNKS, 4)),
            dma((CHUNKS, 2)),
        ],
        compiler_params=pltpu.CompilerParams(
            collective_id=capacity, has_side_effects=True, vmem_limit_bytes=56 * 2**20
        ),
        name=f"exchange_{capacity}",
    )(table, coef, deltas, params, momentum)


def tables_kernel(list_ref, hosting_ref, counts_ref, table_ref, coef_ref):
    f32, bf16 = jnp.float32, jnp.bfloat16
    replica = lax.axis_index("replica")

    def iota(shape, axis):
        return lax.broadcasted_iota(jnp.int32, shape, axis)

    def product(left, right, transposed=False):
        return lax.dot_general(
            left.astype(bf16), right.astype(bf16), (((1,), (1 if transposed else 0,)), ((), ())), preferred_element_type=f32
        )

    def as_float(condition):
        return jnp.where(condition, 1.0, 0.0).astype(f32)

    row, col = iota((128, 128), 0), iota((128, 128), 1)
    row8, col8 = iota((8, 128), 0), iota((8, 128), 1)

    def pick_row(array, i):
        return jnp.sum(jnp.where(row8 == i, array, 0.0), axis=0, keepdims=True)

    spread = product(hosting_ref[...].astype(f32), as_float(iota((16, 128), 1) // 8 == iota((16, 128), 0)))
    own_expert = iota((64, 128), 1) % 8 == iota((64, 128), 0) % 8
    hosted = jnp.sum(jnp.where(own_expert, spread, 0.0).reshape(8, 8, 128), axis=1)
    weight = hosted * counts_ref[...].astype(f32)
    totals = jnp.maximum(jnp.sum(weight, axis=0, keepdims=True), 1.0)
    ratio = weight / totals

    entry = iota((8, SLOTS), 1).astype(f32)
    ones_and_entries = jnp.where(iota((8, SLOTS), 0) == 0, 1.0, entry)
    blocks = iota((BLOCKS, SLOTS), 0)

    member = jnp.concatenate(
        [
            product(ones_and_entries, as_float(blocks == list_ref[r : r + 1, :]), transposed=True)[0:1]
            for r in range(REPLICAS)
        ],
        axis=0,
    )
    mine = list_ref[pl.ds(replica, 1), :]
    listed = as_float(blocks == mine)
    entry_of = product(ones_and_entries, listed, transposed=True)[1:2]

    rank = product(member, as_float((row // OWN == col // OWN) & (row < col)))
    coef_ref[0:8, :] = jnp.where(rank < 0.5, ratio, 0.0)
    coef_ref[8:16, :] = jnp.where(rank > 0.5, ratio, 0.0)

    my_rank = pick_row(rank, replica)
    source = entry_of * pick_row(member, replica)
    by_rank = jnp.where((row8 == 0) == (my_rank < 0.5), source, 0.0)
    index = product(by_rank, as_float(row // OWN == col))

    union = jnp.concatenate(
        [jnp.maximum(member[2 * y : 2 * y + 1], member[2 * y + 1 : 2 * y + 2]) for y in range(4)] * 2, axis=0
    )
    place = product(union, as_float((row // 32 == col // 32) & (row < col)))
    my_place = pick_row(place, replica // 2)
    entry_place = product(jnp.broadcast_to(my_place, (8, BLOCKS)), listed)
    most = jnp.max(jnp.where(union > 0.5, place + 1.0, 0.0), keepdims=True)

    table_ref[0:8, :] = index.astype(jnp.int32)
    table_ref[2:3, 0:SLOTS] = jnp.where(mine >= 0, entry_place[0:1].astype(jnp.int32), -1)
    table_ref[3:4, 0:SLOTS] = jnp.maximum(mine, 0) // 32
    table_ref[4:5, :] = jnp.broadcast_to(most.astype(jnp.int32), (1, 128))
    group = jnp.where(col8 // 32 == row8, (col8 % 32).astype(f32), 0.0)
    for y in range(4):
        holds = as_float((place[y : y + 1] == row.astype(f32)) & (union[y : y + 1] > 0.5))
        table_ref[8 + 4 * y : 12 + 4 * y, :] = product(group, holds, transposed=True)[0:4].astype(jnp.int32)


def tables(block_list, hosting, counts):
    return pl.pallas_call(
        tables_kernel,
        out_shape=(jax.ShapeDtypeStruct((24, 128), jnp.int32), jax.ShapeDtypeStruct((16, 128), jnp.float32)),
        name="tables",
    )(block_list, hosting.transpose(0, 2, 1).reshape(64, 16), counts)


def per_device(deltas, block_list, hosting, counts, params, momentum):
    table, coef = tables(block_list, hosting, counts)
    small, full = (functools.partial(exchange, capacity) for capacity in (20, 32))
    return lax.cond(table[4, 0] <= 20, small, full, table, coef, deltas, params, momentum)


def solution(mesh):
    blocks = P("shard", "replica", None)
    entries = P("replica", None, "shard", None)
    return jax.shard_map(
        per_device,
        mesh=mesh,
        in_specs=(entries, P(), P(), P(), blocks, blocks),
        out_specs=(blocks, blocks, entries),
        check_vma=False,
    )
```

```python
import functools
import math

import jax
import jax.numpy as jnp
from jax import lax
from jax.experimental import pallas as pl
from jax.experimental.pallas import tpu as pltpu
from jax.sharding import PartitionSpec as P

D = 6144
ROWS = 128
HALF = D // 2
CHUNKS = 8
EARLY = 1
DC = HALF // CHUNKS
SLOTS = 64
OWN = 4
CAP = 2
REPLICAS = 8
BLOCKS = 128
MESH = pl.DeviceIdType.MESH

decay_rate = 0.9
outer_rate = 0.7
limit_ratio = 0.1


class Place:
    def __init__(self):
        self.replica = lax.axis_index("replica")
        self.shard = lax.axis_index("shard")
        self.y = self.replica // 2
        self.c = self.replica % 2
        self.x = self.shard // 8
        self.z = self.shard % 8
        self.zh = self.z // 4
        self.zl = self.z % 4
        self.self_xy = self.x == self.y
        self.self_z = self.c == self.zh

    def xy_target(self, dx, dc):
        xt = lax.rem(self.x + dx, 4)
        ct = lax.rem(self.c + dc, 2)
        return xt, ct, (2 * self.x + ct, xt * 8 + self.z)

    def xy_source(self, d):
        r = lax.rem(self.replica + d, 8)
        return r, (r, self.y * 8 + self.z)

    def z_target(self, dz):
        zt = lax.rem(self.z + dz, 8)
        return zt, (2 * self.y + self.zh, self.x * 8 + zt)

    def z_source(self, d, dc):
        zs = lax.rem(self.zl + d, 4)
        cs = lax.rem(self.c + dc, 2)
        return zs, cs, (2 * self.y + cs, self.x * 8 + self.c * 4 + zs)

    def shifted(self, dx, dy, dz, dc):
        x = lax.rem(self.x + dx, 4)
        y = lax.rem(self.y + dy, 4)
        z = lax.rem(self.z + dz, 8)
        c = lax.rem(self.c + dc, 2)
        return (y * 2 + c, x * 8 + z)


def columns(half, n):
    return pl.ds(pl.multiple_of(half * HALF + n * DC, 128), DC)


def guarded(maybe_self, condition, act):
    if maybe_self:
        pl.when(jnp.logical_not(condition))(act)
    else:
        act()


def exchange_kernel(
    capacity, table_ref, coef_ref, deltas_ref, params_ref, momentum_ref,
    new_params_ref, new_momentum_ref, host_ref, *scratch,
):
    (
        packed, rx, sums, gx, sq_cx, sq_y, sq_z, params, momentum, new_params, new_momentum,
        kept, base, picked, relay, host,
    ) = scratch[:16]
    blocks = scratch[16 : 16 + CHUNKS]
    near = scratch[16 + CHUNKS : 16 + 2 * CHUNKS]
    far = scratch[16 + 2 * CHUNKS : 16 + 3 * CHUNKS]
    raw = scratch[16 + 3 * CHUNKS : 16 + 4 * CHUNKS]
    (
        load_sem, raw_sem, xy_send, xy_recv, z_send, z_recv, sq_send, sq_recv,
        a_send, a_recv, y_send, y_recv, x_send, x_recv, d_send, d_recv, host_sem, store_sem,
    ) = scratch[16 + 4 * CHUNKS :]
    me = Place()
    sibling = (2 * me.y + 1 - me.c, me.shard)

    def raw_copy(n, half):
        return pltpu.make_async_copy(
            deltas_ref.at[0, :, :, columns(half, n)], raw[n].at[half], raw_sem.at[n, half]
        )

    for n in range(CHUNKS):
        for half in range(2):
            raw_copy(n, half).start()
    load_params = pltpu.make_async_copy(params_ref, params, load_sem.at[0])
    load_momentum = pltpu.make_async_copy(momentum_ref, momentum, load_sem.at[1])
    load_params.start()
    load_momentum.start()

    barrier = pltpu.get_barrier_semaphore()

    def greet(device):
        pl.semaphore_signal(barrier, inc=1, device_id=device, device_id_type=MESH)

    for d in range(8):
        guarded(d == 0, me.self_xy, functools.partial(greet, me.xy_source(d)[1]))
        guarded(d == 0, me.self_z, functools.partial(greet, me.z_target(d)[1]))
    for d in range(4):
        for dc in range(2):
            guarded(d == 0 and dc == 0, me.self_z, functools.partial(greet, me.z_source(d, dc)[2]))
    stages = (
        (sq_cx, 2 * me.x + me.c, [(d, 0, 0, c) for d in (2, 1, 3, 0) for c in (0, 1) if d or c]),
        (sq_y, me.y, [(0, d, 0, 0) for d in (1, 2, 3)]),
        (sq_z, me.z, [(0, 0, d, 0) for d in range(1, 8)]),
    )
    for _, _, offsets in stages:
        for offset in offsets:
            greet(me.shifted(*offset))

    def pack(n):
        for half in range(2):
            raw_copy(n, half).wait()

        def place(owner, carry):
            for k in range(CAP):
                entry = table_ref[k, owner]
                for half in range(2):
                    packed[n, half, owner * CAP + k] = raw[n][half, entry]
            return carry

        lax.fori_loop(0, 32, place, 0)

    pack(0)
    pl.semaphore_wait(
        barrier,
        8 + 16 + 17 - me.self_xy.astype(jnp.int32) - 2 * me.self_z.astype(jnp.int32),
    )

    def xy_copy(n, dx, dc):
        xt, ct, device = me.xy_target(dx, dc)
        return pltpu.make_async_remote_copy(
            src_ref=packed.at[n, ct, pl.ds(xt * 16, 16)],
            dst_ref=rx.at[n, me.replica],
            send_sem=xy_send.at[n, dx * 2 + dc],
            recv_sem=xy_recv.at[n, me.replica],
            device_id=device,
            device_id_type=MESH,
        )

    def xy_arrival(n, d):
        r, device = me.xy_source(d)
        return pltpu.make_async_remote_copy(
            src_ref=packed.at[n, 0, pl.ds(0, 16)],
            dst_ref=rx.at[n, r],
            send_sem=xy_send.at[n, 0],
            recv_sem=xy_recv.at[n, r],
            device_id=device,
            device_id_type=MESH,
        )

    def z_copy(n, dz):
        zt, device = me.z_target(dz)
        return pltpu.make_async_remote_copy(
            src_ref=sums.at[n, pl.ds(zt * 4, 4)],
            dst_ref=gx.at[n, me.zl * 2 + me.c],
            send_sem=z_send.at[n, dz],
            recv_sem=z_recv.at[n, me.zl * 2 + me.c],
            device_id=device,
            device_id_type=MESH,
        )

    def z_arrival(n, d, dc):
        zs, cs, device = me.z_source(d, dc)
        return pltpu.make_async_remote_copy(
            src_ref=sums.at[n, pl.ds(0, 4)],
            dst_ref=gx.at[n, zs * 2 + cs],
            send_sem=z_send.at[n, 0],
            recv_sem=z_recv.at[n, zs * 2 + cs],
            device_id=device,
            device_id_type=MESH,
        )

    xy_order = [(1, 0), (2, 0), (0, 0), (3, 0), (1, 1), (2, 1), (0, 1), (3, 1)]
    z_order = [4, 3, 5, 2, 6, 1, 7, 0]

    def start_z(n):
        for dz in z_order:
            guarded(dz == 0, me.self_z, lambda dz=dz: z_copy(n, dz).start())

    def a_copy(n, d, dc):
        zt, ct, device = me.z_source(d, dc)
        return pltpu.make_async_remote_copy(
            src_ref=kept.at[n, ct, zt],
            dst_ref=base.at[n, pl.ds(me.z * OWN, OWN)],
            send_sem=a_send.at[n, d * 2 + dc],
            recv_sem=a_recv.at[n, me.z],
            device_id=device,
            device_id_type=MESH,
        )

    def a_arrival(n, dz):
        zs, device = me.z_target(dz)
        return pltpu.make_async_remote_copy(
            src_ref=kept.at[n, 0, 0],
            dst_ref=base.at[n, pl.ds(zs * OWN, OWN)],
            send_sem=a_send.at[n, 0],
            recv_sem=a_recv.at[n, zs],
            device_id=device,
            device_id_type=MESH,
        )

    a_order = [(d, dc) for d in (2, 1, 3, 0) for dc in (0, 1)]
    for n in range(CHUNKS):
        if n > 0:
            pack(n)
        for dx, dc in xy_order:
            guarded(dx == 0 and dc == 0, me.self_xy, lambda n=n, dx=dx, dc=dc: xy_copy(n, dx, dc).start())

        @pl.when(me.self_xy)
        def _(n=n):
            def own(k, carry):
                rx[n, me.replica, k] = packed[n, me.c, me.x * 16 + k]
                return carry

            lax.fori_loop(0, 16, own, 0)

        if n == 0:
            load_params.wait()
            load_momentum.wait()
        for half in range(2):
            wide = slice(half * HALF + n * DC, half * HALF + n * DC + DC)
            for pair in range(2):
                rows = slice(pair * 8, pair * 8 + 8)
                for j in range(OWN):
                    keep = params[j, rows, wide] - (outer_rate * decay_rate**2) * momentum[j, rows, wide]
                    kept[n, half, pair * 2, j] = keep[0:4]
                    kept[n, half, pair * 2 + 1, j] = keep[4:8]
        for d, dc in a_order:
            guarded(d == 0 and dc == 0, me.self_z, lambda n=n, d=d, dc=dc: a_copy(n, d, dc).start())

        @pl.when(me.self_z)
        def _(n=n):
            for j in range(OWN):
                base[n, me.z * OWN + j] = kept[n, me.c, me.zl, j]

    total = jnp.zeros((4, DC), jnp.float32)
    for n in range(CHUNKS):
        for d in range(8):
            guarded(d == 0, me.self_xy, lambda n=n, d=d: xy_arrival(n, d).wait_recv())

        def mix(owner, total, n=n):
            acc = [jnp.zeros((4, DC), jnp.float32) for _ in range(OWN)]
            for r in range(REPLICAS):
                for k in range(CAP):
                    rows = rx[n, r, owner * CAP + k].astype(jnp.float32)
                    for j in range(OWN):
                        acc[j] = acc[j] + coef_ref[k * REPLICAS + r, me.x * 32 + owner * OWN + j] * rows
            for j in range(OWN):
                sums[n, owner * OWN + j] = acc[j]
                total = total + acc[j] * acc[j]
            return total

        total = lax.fori_loop(0, 8, mix, total)
        if n < EARLY:
            start_z(n)

        @pl.when(me.self_z)
        def _(n=n):
            for j in range(OWN):
                gx[n, me.zl * 2 + me.c, j] = sums[n, me.z * OWN + j]

    value = jnp.full((8, 128), jnp.sum(total), jnp.float32)
    first = 0
    for slots, mine, offsets in stages:
        slots[mine] = value
        copies = []
        for i, offset in enumerate(offsets):
            copy = pltpu.make_async_remote_copy(
                src_ref=slots.at[mine],
                dst_ref=slots.at[mine],
                send_sem=sq_send.at[first + i],
                recv_sem=sq_recv.at[first + i],
                device_id=me.shifted(*offset),
                device_id_type=MESH,
            )
            copy.start()
            copies.append(copy)
        if slots is sq_z:
            for n in range(EARLY, CHUNKS):
                start_z(n)
        for copy in copies:
            copy.wait()
        value = slots[0]
        for i in range(1, slots.shape[0]):
            value = value + slots[i]
        first += len(offsets)

    limit = limit_ratio * math.sqrt(BLOCKS * ROWS * D)
    factor = jnp.minimum(1.0, limit / jnp.sqrt(value + 1e-06))[0:1, 0:1]
    step_size = (outer_rate * (1.0 + decay_rate)) * factor

    def store_copies(n):
        copies = []
        for half in range(2):
            wide = slice(half * HALF + n * DC, half * HALF + n * DC + DC)
            for i, (inside, outside) in enumerate(
                ((new_params, new_params_ref), (new_momentum, new_momentum_ref))
            ):
                copies.append(
                    pltpu.make_async_copy(
                        inside.at[:, :, wide], outside.at[:, :, wide], store_sem.at[n, half * 2 + i]
                    )
                )
        return copies

    def update(n):
        for d in range(4):
            for dc in range(2):
                guarded(d == 0 and dc == 0, me.self_z, lambda d=d, dc=dc: z_arrival(n, d, dc).wait_recv())
        for half in range(2):
            wide = slice(half * HALF + n * DC, half * HALF + n * DC + DC)
            for pair in range(2):
                rows = slice(pair * 8, pair * 8 + 8)
                for j in range(OWN):
                    grad = jnp.concatenate([gx[n, pair * 4 + half, j], gx[n, pair * 4 + 2 + half, j]], axis=0)
                    scaled = factor * grad
                    moved = decay_rate * momentum[j, rows, wide] + scaled
                    new_momentum[j, rows, wide] = moved
                    new_params[j, rows, wide] = params[j, rows, wide] - outer_rate * (scaled + decay_rate * moved)
        for copy in store_copies(n):
            copy.start()

    def y_copy(n, d, arrival=False):
        ys = lax.rem(me.y + d, 4) if arrival else me.y
        return pltpu.make_async_remote_copy(
            src_ref=picked.at[n, d - 1],
            dst_ref=relay.at[n, ys],
            send_sem=y_send.at[n, d],
            recv_sem=y_recv.at[n, ys],
            device_id=me.shifted(0, d, 0, 0),
            device_id_type=MESH,
        )

    def x_copy(n, d, arrival=False):
        xs = lax.rem(me.x + d, 4)
        xd = xs if arrival else me.x
        return pltpu.make_async_remote_copy(
            src_ref=relay.at[n, xs],
            dst_ref=near[n].at[pl.ds(xd * capacity, capacity)],
            send_sem=x_send.at[n, d],
            recv_sem=x_recv.at[n, xd],
            device_id=me.shifted(d, 0, 0, 0),
            device_id_type=MESH,
        )

    def d_copy(n, d):
        xs = lax.rem(me.x + d, 4)
        return pltpu.make_async_remote_copy(
            src_ref=near[n].at[pl.ds(xs * capacity, capacity)],
            dst_ref=far[n].at[pl.ds(xs * capacity, capacity)],
            send_sem=d_send.at[n, xs],
            recv_sem=d_recv.at[n, xs],
            device_id=sibling,
            device_id_type=MESH,
        )

    def host_copy(n, half):
        return pltpu.make_async_copy(
            host.at[:, :, columns(half, n)], host_ref.at[0, :, :, columns(half, n)], host_sem.at[n, half]
        )

    order = (2, 1, 3)

    def start_y(n):
        for dz in range(8):
            guarded(dz == 0, me.self_z, lambda dz=dz: a_arrival(n, dz).wait_recv())

        def fresh(block, carry):
            blocks[n][block] = (base[n, block] - step_size * sums[n, block]).astype(jnp.bfloat16)
            return carry

        lax.fori_loop(0, 32, fresh, 0)

        def pick(k, carry):
            for d in range(1, 4):
                picked[n, d - 1, k] = blocks[n][table_ref[8 + lax.rem(me.y + d, 4) * 4 + me.x, k]]
            relay[n, me.y, k] = blocks[n][table_ref[8 + me.y * 4 + me.x, k]]
            return carry

        lax.fori_loop(0, capacity, pick, 0)
        for d in order:
            y_copy(n, d).start()

    def start_x(n):
        for d in order:
            y_copy(n, d, arrival=True).wait_recv()
        for d in order:
            x_copy(n, d).start()

        def own(k, carry):
            near[n][me.x * capacity + k] = relay[n, me.x, k]
            return carry

        lax.fori_loop(0, capacity, own, 0)

    def start_d(n):
        d_copy(n, 0).start()
        for d in order:
            x_copy(n, d, arrival=True).wait_recv()
            d_copy(n, d).start()

    def unpack(n):
        for d in range(4):
            d_copy(n, d).wait_recv()

        def entry(k, carry):
            place = table_ref[2, k]
            safe = table_ref[3, k] * capacity + jnp.maximum(place, 0)
            for rows, half in ((near[n], me.c), (far[n], 1 - me.c)):
                value = rows[safe]
                host[k, :, columns(half, n)] = jnp.where(place >= 0, value, jnp.zeros_like(value))
            return carry

        lax.fori_loop(0, SLOTS, entry, 0)
        for half in range(2):
            host_copy(n, half).start()

    for step in range(CHUNKS + 6):
        for lag, stage in ((0, start_y), (2, start_x), (4, start_d), (5, unpack), (6, update)):
            if 0 <= step - lag < CHUNKS:
                stage(step - lag)

    for n in range(CHUNKS):
        for dx, dc in xy_order:
            guarded(dx == 0 and dc == 0, me.self_xy, lambda n=n, dx=dx, dc=dc: xy_copy(n, dx, dc).wait_send())
        for dz in z_order:
            guarded(dz == 0, me.self_z, lambda n=n, dz=dz: z_copy(n, dz).wait_send())
        for d, dc in a_order:
            guarded(d == 0 and dc == 0, me.self_z, lambda n=n, d=d, dc=dc: a_copy(n, d, dc).wait_send())
        for d in order:
            y_copy(n, d).wait_send()
            x_copy(n, d).wait_send()
        for d in range(4):
            d_copy(n, d).wait_send()
    for n in range(CHUNKS):
        for copy in store_copies(n):
            copy.wait()
        for half in range(2):
            host_copy(n, half).wait()


def exchange(capacity, table, coef, deltas, params, momentum):
    vmem, dma = pltpu.VMEM, pltpu.SemaphoreType.DMA
    smem, anywhere = pl.BlockSpec(memory_space=pltpu.SMEM), pl.BlockSpec(memory_space=pl.ANY)
    owned = jax.ShapeDtypeStruct((OWN, 16, D), jnp.float32)
    return pl.pallas_call(
        functools.partial(exchange_kernel, capacity),
        out_shape=(owned, owned, jax.ShapeDtypeStruct((1, SLOTS, 4, D), jnp.bfloat16)),
        in_specs=[smem, smem, anywhere, anywhere, anywhere],
        out_specs=(anywhere, anywhere, anywhere),
        scratch_shapes=[
            vmem((CHUNKS, 2, SLOTS, 4, DC), jnp.bfloat16),
            vmem((CHUNKS, REPLICAS, 16, 4, DC), jnp.bfloat16),
            vmem((CHUNKS, 32, 4, DC), jnp.float32),
            vmem((CHUNKS, 8, OWN, 4, DC), jnp.float32),
            vmem((8, 8, 128), jnp.float32),
            vmem((4, 8, 128), jnp.float32),
            vmem((8, 8, 128), jnp.float32),
            vmem((OWN, 16, D), jnp.float32),
            vmem((OWN, 16, D), jnp.float32),
            vmem((OWN, 16, D), jnp.float32),
            vmem((OWN, 16, D), jnp.float32),
            vmem((CHUNKS, 2, 4, OWN, 4, DC), jnp.float32),
            vmem((CHUNKS, 32, 4, DC), jnp.float32),
            vmem((CHUNKS, 3, capacity, 4, DC), jnp.bfloat16),
            vmem((CHUNKS, 4, capacity, 4, DC), jnp.bfloat16),
            vmem((SLOTS, 4, D), jnp.bfloat16),
        ]
        + [vmem((32, 4, DC), jnp.bfloat16)] * CHUNKS
        + [vmem((4 * capacity, 4, DC), jnp.bfloat16)] * (2 * CHUNKS)
        + [vmem((2, SLOTS, 4, DC), jnp.bfloat16)] * CHUNKS
        + [
            dma((2,)),
            dma((CHUNKS, 2)),
            dma((CHUNKS, 8)),
            dma((CHUNKS, 8)),
            dma((CHUNKS, 8)),
            dma((CHUNKS, 8)),
            dma((17,)),
            dma((17,)),
            dma((CHUNKS, 8)),
            dma((CHUNKS, 8)),
            dma((CHUNKS, 4)),
            dma((CHUNKS, 4)),
            dma((CHUNKS, 4)),
            dma((CHUNKS, 4)),
            dma((CHUNKS, 4)),
            dma((CHUNKS, 4)),
            dma((CHUNKS, 2)),
            dma((CHUNKS, 4)),
        ],
        compiler_params=pltpu.CompilerParams(
            collective_id=capacity, has_side_effects=True, vmem_limit_bytes=56 * 2**20
        ),
        name=f"exchange_{capacity}",
    )(table, coef, deltas, params, momentum)


def tables_kernel(list_ref, hosting_ref, counts_ref, table_ref, coef_ref):
    f32, bf16 = jnp.float32, jnp.bfloat16
    replica = lax.axis_index("replica")

    def iota(shape, axis):
        return lax.broadcasted_iota(jnp.int32, shape, axis)

    def product(left, right, transposed=False):
        return lax.dot_general(
            left.astype(bf16), right.astype(bf16), (((1,), (1 if transposed else 0,)), ((), ())), preferred_element_type=f32
        )

    def as_float(condition):
        return jnp.where(condition, 1.0, 0.0).astype(f32)

    row, col = iota((128, 128), 0), iota((128, 128), 1)
    row8, col8 = iota((8, 128), 0), iota((8, 128), 1)

    def pick_row(array, i):
        return jnp.sum(jnp.where(row8 == i, array, 0.0), axis=0, keepdims=True)

    spread = product(hosting_ref[...].astype(f32), as_float(iota((16, 128), 1) // 8 == iota((16, 128), 0)))
    own_expert = iota((64, 128), 1) % 8 == iota((64, 128), 0) % 8
    hosted = jnp.sum(jnp.where(own_expert, spread, 0.0).reshape(8, 8, 128), axis=1)
    weight = hosted * counts_ref[...].astype(f32)
    totals = jnp.maximum(jnp.sum(weight, axis=0, keepdims=True), 1.0)
    ratio = weight / totals

    entry = iota((8, SLOTS), 1).astype(f32)
    ones_and_entries = jnp.where(iota((8, SLOTS), 0) == 0, 1.0, entry)
    blocks = iota((BLOCKS, SLOTS), 0)

    member = jnp.concatenate(
        [
            product(ones_and_entries, as_float(blocks == list_ref[r : r + 1, :]), transposed=True)[0:1]
            for r in range(REPLICAS)
        ],
        axis=0,
    )
    mine = list_ref[pl.ds(replica, 1), :]
    listed = as_float(blocks == mine)
    entry_of = product(ones_and_entries, listed, transposed=True)[1:2]

    rank = product(member, as_float((row // OWN == col // OWN) & (row < col)))
    coef_ref[0:8, :] = jnp.where(rank < 0.5, ratio, 0.0)
    coef_ref[8:16, :] = jnp.where(rank > 0.5, ratio, 0.0)

    my_rank = pick_row(rank, replica)
    source = entry_of * pick_row(member, replica)
    by_rank = jnp.where((row8 == 0) == (my_rank < 0.5), source, 0.0)
    index = product(by_rank, as_float(row // OWN == col))

    union = jnp.concatenate(
        [jnp.maximum(member[2 * y : 2 * y + 1], member[2 * y + 1 : 2 * y + 2]) for y in range(4)] * 2, axis=0
    )
    place = product(union, as_float((row // 32 == col // 32) & (row < col)))
    my_place = pick_row(place, replica // 2)
    entry_place = product(jnp.broadcast_to(my_place, (8, BLOCKS)), listed)
    most = jnp.max(jnp.where(union > 0.5, place + 1.0, 0.0), keepdims=True)

    table_ref[0:8, :] = index.astype(jnp.int32)
    table_ref[2:3, 0:SLOTS] = jnp.where(mine >= 0, entry_place[0:1].astype(jnp.int32), -1)
    table_ref[3:4, 0:SLOTS] = jnp.maximum(mine, 0) // 32
    table_ref[4:5, :] = jnp.broadcast_to(most.astype(jnp.int32), (1, 128))
    group = jnp.where(col8 // 32 == row8, (col8 % 32).astype(f32), 0.0)
    for y in range(4):
        holds = as_float((place[y : y + 1] == row.astype(f32)) & (union[y : y + 1] > 0.5))
        table_ref[8 + 4 * y : 12 + 4 * y, :] = product(group, holds, transposed=True)[0:4].astype(jnp.int32)


def tables(block_list, hosting, counts):
    return pl.pallas_call(
        tables_kernel,
        out_shape=(jax.ShapeDtypeStruct((24, 128), jnp.int32), jax.ShapeDtypeStruct((16, 128), jnp.float32)),
        name="tables",
    )(block_list, hosting.transpose(0, 2, 1).reshape(64, 16), counts)


def per_device(deltas, block_list, hosting, counts, params, momentum):
    table, coef = tables(block_list, hosting, counts)
    small, full = (functools.partial(exchange, capacity) for capacity in (20, 32))
    return lax.cond(table[4, 0] <= 20, small, full, table, coef, deltas, params, momentum)


def solution(mesh):
    blocks = P("shard", "replica", None)
    entries = P("replica", None, "shard", None)
    return jax.shard_map(
        per_device,
        mesh=mesh,
        in_specs=(entries, P(), P(), P(), blocks, blocks),
        out_specs=(blocks, blocks, entries),
        check_vma=False,
    )
```

```python
import functools
import math

import jax
import jax.numpy as jnp
from jax import lax
from jax.experimental import pallas as pl
from jax.experimental.pallas import tpu as pltpu
from jax.sharding import PartitionSpec as P

D = 6144
ROWS = 128
HALF = D // 2
CHUNKS = 6
EARLY = 1
DC = HALF // CHUNKS
SLOTS = 64
OWN = 4
CAP = 2
REPLICAS = 8
BLOCKS = 128
MESH = pl.DeviceIdType.MESH

decay_rate = 0.9
outer_rate = 0.7
limit_ratio = 0.1


class Place:
    def __init__(self):
        self.replica = lax.axis_index("replica")
        self.shard = lax.axis_index("shard")
        self.y = self.replica // 2
        self.c = self.replica % 2
        self.x = self.shard // 8
        self.z = self.shard % 8
        self.zh = self.z // 4
        self.zl = self.z % 4
        self.self_xy = self.x == self.y
        self.self_z = self.c == self.zh

    def xy_target(self, dx, dc):
        xt = lax.rem(self.x + dx, 4)
        ct = lax.rem(self.c + dc, 2)
        return xt, ct, (2 * self.x + ct, xt * 8 + self.z)

    def xy_source(self, d):
        r = lax.rem(self.replica + d, 8)
        return r, (r, self.y * 8 + self.z)

    def z_target(self, dz):
        zt = lax.rem(self.z + dz, 8)
        return zt, (2 * self.y + self.zh, self.x * 8 + zt)

    def z_source(self, d, dc):
        zs = lax.rem(self.zl + d, 4)
        cs = lax.rem(self.c + dc, 2)
        return zs, cs, (2 * self.y + cs, self.x * 8 + self.c * 4 + zs)

    def shifted(self, dx, dy, dz, dc):
        x = lax.rem(self.x + dx, 4)
        y = lax.rem(self.y + dy, 4)
        z = lax.rem(self.z + dz, 8)
        c = lax.rem(self.c + dc, 2)
        return (y * 2 + c, x * 8 + z)


def columns(half, n):
    return pl.ds(pl.multiple_of(half * HALF + n * DC, 128), DC)


def guarded(maybe_self, condition, act):
    if maybe_self:
        pl.when(jnp.logical_not(condition))(act)
    else:
        act()


def exchange_kernel(
    capacity, table_ref, coef_ref, deltas_ref, params_ref, momentum_ref,
    new_params_ref, new_momentum_ref, host_ref, *scratch,
):
    (
        packed, rx, sums, gx, sq_cx, sq_y, sq_z, params, momentum, new_params, new_momentum,
        kept, base, picked, relay, host,
    ) = scratch[:16]
    blocks = scratch[16 : 16 + CHUNKS]
    near = scratch[16 + CHUNKS : 16 + 2 * CHUNKS]
    far = scratch[16 + 2 * CHUNKS : 16 + 3 * CHUNKS]
    raw = scratch[16 + 3 * CHUNKS : 16 + 4 * CHUNKS]
    (
        load_sem, raw_sem, xy_send, xy_recv, z_send, z_recv, sq_send, sq_recv,
        a_send, a_recv, y_send, y_recv, x_send, x_recv, d_send, d_recv, host_sem, store_sem,
    ) = scratch[16 + 4 * CHUNKS :]
    me = Place()
    sibling = (2 * me.y + 1 - me.c, me.shard)

    def raw_copy(n, half):
        return pltpu.make_async_copy(
            deltas_ref.at[0, :, :, columns(half, n)], raw[n].at[half], raw_sem.at[n, half]
        )

    for n in range(CHUNKS):
        for half in range(2):
            raw_copy(n, half).start()
    load_params = pltpu.make_async_copy(params_ref, params, load_sem.at[0])
    load_momentum = pltpu.make_async_copy(momentum_ref, momentum, load_sem.at[1])
    load_params.start()
    load_momentum.start()

    barrier = pltpu.get_barrier_semaphore()

    def greet(device):
        pl.semaphore_signal(barrier, inc=1, device_id=device, device_id_type=MESH)

    for d in range(8):
        guarded(d == 0, me.self_xy, functools.partial(greet, me.xy_source(d)[1]))
        guarded(d == 0, me.self_z, functools.partial(greet, me.z_target(d)[1]))
    for d in range(4):
        for dc in range(2):
            guarded(d == 0 and dc == 0, me.self_z, functools.partial(greet, me.z_source(d, dc)[2]))
    stages = (
        (sq_cx, 2 * me.x + me.c, [(d, 0, 0, c) for d in (2, 1, 3, 0) for c in (0, 1) if d or c]),
        (sq_y, me.y, [(0, d, 0, 0) for d in (1, 2, 3)]),
        (sq_z, me.z, [(0, 0, d, 0) for d in range(1, 8)]),
    )
    for _, _, offsets in stages:
        for offset in offsets:
            greet(me.shifted(*offset))

    def pack(n):
        for half in range(2):
            raw_copy(n, half).wait()

        def place(owner, carry):
            for k in range(CAP):
                entry = table_ref[k, owner]
                for half in range(2):
                    packed[n, half, owner * CAP + k] = raw[n][half, entry]
            return carry

        lax.fori_loop(0, 32, place, 0)

    pack(0)
    pl.semaphore_wait(
        barrier,
        8 + 16 + 17 - me.self_xy.astype(jnp.int32) - 2 * me.self_z.astype(jnp.int32),
    )

    def xy_copy(n, dx, dc):
        xt, ct, device = me.xy_target(dx, dc)
        return pltpu.make_async_remote_copy(
            src_ref=packed.at[n, ct, pl.ds(xt * 16, 16)],
            dst_ref=rx.at[n, me.replica],
            send_sem=xy_send.at[n, dx * 2 + dc],
            recv_sem=xy_recv.at[n, me.replica],
            device_id=device,
            device_id_type=MESH,
        )

    def xy_arrival(n, d):
        r, device = me.xy_source(d)
        return pltpu.make_async_remote_copy(
            src_ref=packed.at[n, 0, pl.ds(0, 16)],
            dst_ref=rx.at[n, r],
            send_sem=xy_send.at[n, 0],
            recv_sem=xy_recv.at[n, r],
            device_id=device,
            device_id_type=MESH,
        )

    def z_copy(n, dz):
        zt, device = me.z_target(dz)
        return pltpu.make_async_remote_copy(
            src_ref=sums.at[n, pl.ds(zt * 4, 4)],
            dst_ref=gx.at[n, me.zl * 2 + me.c],
            send_sem=z_send.at[n, dz],
            recv_sem=z_recv.at[n, me.zl * 2 + me.c],
            device_id=device,
            device_id_type=MESH,
        )

    def z_arrival(n, d, dc):
        zs, cs, device = me.z_source(d, dc)
        return pltpu.make_async_remote_copy(
            src_ref=sums.at[n, pl.ds(0, 4)],
            dst_ref=gx.at[n, zs * 2 + cs],
            send_sem=z_send.at[n, 0],
            recv_sem=z_recv.at[n, zs * 2 + cs],
            device_id=device,
            device_id_type=MESH,
        )

    xy_order = [(1, 0), (2, 0), (0, 0), (3, 0), (1, 1), (2, 1), (0, 1), (3, 1)]
    z_order = [4, 3, 5, 2, 6, 1, 7, 0]

    def start_z(n):
        for dz in z_order:
            guarded(dz == 0, me.self_z, lambda dz=dz: z_copy(n, dz).start())

    def a_copy(n, d, dc):
        zt, ct, device = me.z_source(d, dc)
        return pltpu.make_async_remote_copy(
            src_ref=kept.at[n, ct, zt],
            dst_ref=base.at[n, pl.ds(me.z * OWN, OWN)],
            send_sem=a_send.at[n, d * 2 + dc],
            recv_sem=a_recv.at[n, me.z],
            device_id=device,
            device_id_type=MESH,
        )

    def a_arrival(n, dz):
        zs, device = me.z_target(dz)
        return pltpu.make_async_remote_copy(
            src_ref=kept.at[n, 0, 0],
            dst_ref=base.at[n, pl.ds(zs * OWN, OWN)],
            send_sem=a_send.at[n, 0],
            recv_sem=a_recv.at[n, zs],
            device_id=device,
            device_id_type=MESH,
        )

    a_order = [(d, dc) for d in (2, 1, 3, 0) for dc in (0, 1)]
    for n in range(CHUNKS):
        if n > 0:
            pack(n)
        for dx, dc in xy_order:
            guarded(dx == 0 and dc == 0, me.self_xy, lambda n=n, dx=dx, dc=dc: xy_copy(n, dx, dc).start())

        @pl.when(me.self_xy)
        def _(n=n):
            def own(k, carry):
                rx[n, me.replica, k] = packed[n, me.c, me.x * 16 + k]
                return carry

            lax.fori_loop(0, 16, own, 0)

        if n == 0:
            load_params.wait()
            load_momentum.wait()
        for half in range(2):
            wide = slice(half * HALF + n * DC, half * HALF + n * DC + DC)
            for pair in range(2):
                rows = slice(pair * 8, pair * 8 + 8)
                for j in range(OWN):
                    keep = params[j, rows, wide] - (outer_rate * decay_rate**2) * momentum[j, rows, wide]
                    kept[n, half, pair * 2, j] = keep[0:4]
                    kept[n, half, pair * 2 + 1, j] = keep[4:8]
        for d, dc in a_order:
            guarded(d == 0 and dc == 0, me.self_z, lambda n=n, d=d, dc=dc: a_copy(n, d, dc).start())

        @pl.when(me.self_z)
        def _(n=n):
            for j in range(OWN):
                base[n, me.z * OWN + j] = kept[n, me.c, me.zl, j]

    total = jnp.zeros((4, DC), jnp.float32)
    for n in range(CHUNKS):
        for d in range(8):
            guarded(d == 0, me.self_xy, lambda n=n, d=d: xy_arrival(n, d).wait_recv())

        def mix(owner, total, n=n):
            acc = [jnp.zeros((4, DC), jnp.float32) for _ in range(OWN)]
            for r in range(REPLICAS):
                for k in range(CAP):
                    rows = rx[n, r, owner * CAP + k].astype(jnp.float32)
                    for j in range(OWN):
                        acc[j] = acc[j] + coef_ref[k * REPLICAS + r, me.x * 32 + owner * OWN + j] * rows
            for j in range(OWN):
                sums[n, owner * OWN + j] = acc[j]
                total = total + acc[j] * acc[j]
            return total

        total = lax.fori_loop(0, 8, mix, total)
        if n < EARLY:
            start_z(n)

        @pl.when(me.self_z)
        def _(n=n):
            for j in range(OWN):
                gx[n, me.zl * 2 + me.c, j] = sums[n, me.z * OWN + j]

    value = jnp.full((8, 128), jnp.sum(total), jnp.float32)
    first = 0
    for slots, mine, offsets in stages:
        slots[mine] = value
        copies = []
        for i, offset in enumerate(offsets):
            copy = pltpu.make_async_remote_copy(
                src_ref=slots.at[mine],
                dst_ref=slots.at[mine],
                send_sem=sq_send.at[first + i],
                recv_sem=sq_recv.at[first + i],
                device_id=me.shifted(*offset),
                device_id_type=MESH,
            )
            copy.start()
            copies.append(copy)
        if slots is sq_z:
            for n in range(EARLY, CHUNKS):
                start_z(n)
        for copy in copies:
            copy.wait()
        value = slots[0]
        for i in range(1, slots.shape[0]):
            value = value + slots[i]
        first += len(offsets)

    limit = limit_ratio * math.sqrt(BLOCKS * ROWS * D)
    factor = jnp.minimum(1.0, limit / jnp.sqrt(value + 1e-06))[0:1, 0:1]
    step_size = (outer_rate * (1.0 + decay_rate)) * factor

    def store_copies(n):
        copies = []
        for half in range(2):
            wide = slice(half * HALF + n * DC, half * HALF + n * DC + DC)
            for i, (inside, outside) in enumerate(
                ((new_params, new_params_ref), (new_momentum, new_momentum_ref))
            ):
                copies.append(
                    pltpu.make_async_copy(
                        inside.at[:, :, wide], outside.at[:, :, wide], store_sem.at[n, half * 2 + i]
                    )
                )
        return copies

    def update(n):
        for d in range(4):
            for dc in range(2):
                guarded(d == 0 and dc == 0, me.self_z, lambda d=d, dc=dc: z_arrival(n, d, dc).wait_recv())
        for half in range(2):
            wide = slice(half * HALF + n * DC, half * HALF + n * DC + DC)
            for pair in range(2):
                rows = slice(pair * 8, pair * 8 + 8)
                for j in range(OWN):
                    grad = jnp.concatenate([gx[n, pair * 4 + half, j], gx[n, pair * 4 + 2 + half, j]], axis=0)
                    scaled = factor * grad
                    moved = decay_rate * momentum[j, rows, wide] + scaled
                    new_momentum[j, rows, wide] = moved
                    new_params[j, rows, wide] = params[j, rows, wide] - outer_rate * (scaled + decay_rate * moved)
        for copy in store_copies(n):
            copy.start()

    def y_copy(n, d, arrival=False):
        ys = lax.rem(me.y + d, 4) if arrival else me.y
        return pltpu.make_async_remote_copy(
            src_ref=picked.at[n, d - 1],
            dst_ref=relay.at[n, ys],
            send_sem=y_send.at[n, d],
            recv_sem=y_recv.at[n, ys],
            device_id=me.shifted(0, d, 0, 0),
            device_id_type=MESH,
        )

    def x_copy(n, d, arrival=False):
        xs = lax.rem(me.x + d, 4)
        xd = xs if arrival else me.x
        return pltpu.make_async_remote_copy(
            src_ref=relay.at[n, xs],
            dst_ref=near[n].at[pl.ds(xd * capacity, capacity)],
            send_sem=x_send.at[n, d],
            recv_sem=x_recv.at[n, xd],
            device_id=me.shifted(d, 0, 0, 0),
            device_id_type=MESH,
        )

    def d_copy(n, d):
        xs = lax.rem(me.x + d, 4)
        return pltpu.make_async_remote_copy(
            src_ref=near[n].at[pl.ds(xs * capacity, capacity)],
            dst_ref=far[n].at[pl.ds(xs * capacity, capacity)],
            send_sem=d_send.at[n, xs],
            recv_sem=d_recv.at[n, xs],
            device_id=sibling,
            device_id_type=MESH,
        )

    def host_copy(n, half):
        return pltpu.make_async_copy(
            host.at[:, :, columns(half, n)], host_ref.at[0, :, :, columns(half, n)], host_sem.at[n, half]
        )

    order = (2, 1, 3)

    def start_y(n):
        for dz in range(8):
            guarded(dz == 0, me.self_z, lambda dz=dz: a_arrival(n, dz).wait_recv())

        def fresh(block, carry):
            blocks[n][block] = (base[n, block] - step_size * sums[n, block]).astype(jnp.bfloat16)
            return carry

        lax.fori_loop(0, 32, fresh, 0)

        def pick(k, carry):
            for d in range(1, 4):
                picked[n, d - 1, k] = blocks[n][table_ref[8 + lax.rem(me.y + d, 4) * 4 + me.x, k]]
            relay[n, me.y, k] = blocks[n][table_ref[8 + me.y * 4 + me.x, k]]
            return carry

        lax.fori_loop(0, capacity, pick, 0)
        for d in order:
            y_copy(n, d).start()

    def start_x(n):
        for d in order:
            y_copy(n, d, arrival=True).wait_recv()
        for d in order:
            x_copy(n, d).start()

        def own(k, carry):
            near[n][me.x * capacity + k] = relay[n, me.x, k]
            return carry

        lax.fori_loop(0, capacity, own, 0)

    def start_d(n):
        d_copy(n, 0).start()
        for d in order:
            x_copy(n, d, arrival=True).wait_recv()
            d_copy(n, d).start()

    def unpack(n):
        for d in range(4):
            d_copy(n, d).wait_recv()

        def entry(k, carry):
            place = table_ref[2, k]
            safe = table_ref[3, k] * capacity + jnp.maximum(place, 0)
            for rows, half in ((near[n], me.c), (far[n], 1 - me.c)):
                value = rows[safe]
                host[k, :, columns(half, n)] = jnp.where(place >= 0, value, jnp.zeros_like(value))
            return carry

        lax.fori_loop(0, SLOTS, entry, 0)
        for half in range(2):
            host_copy(n, half).start()

    for step in range(CHUNKS + 6):
        for lag, stage in ((0, start_y), (2, start_x), (4, start_d), (5, unpack), (6, update)):
            if 0 <= step - lag < CHUNKS:
                stage(step - lag)

    for n in range(CHUNKS):
        for dx, dc in xy_order:
            guarded(dx == 0 and dc == 0, me.self_xy, lambda n=n, dx=dx, dc=dc: xy_copy(n, dx, dc).wait_send())
        for dz in z_order:
            guarded(dz == 0, me.self_z, lambda n=n, dz=dz: z_copy(n, dz).wait_send())
        for d, dc in a_order:
            guarded(d == 0 and dc == 0, me.self_z, lambda n=n, d=d, dc=dc: a_copy(n, d, dc).wait_send())
        for d in order:
            y_copy(n, d).wait_send()
            x_copy(n, d).wait_send()
        for d in range(4):
            d_copy(n, d).wait_send()
    for n in range(CHUNKS):
        for copy in store_copies(n):
            copy.wait()
        for half in range(2):
            host_copy(n, half).wait()


def exchange(capacity, table, coef, deltas, params, momentum):
    vmem, dma = pltpu.VMEM, pltpu.SemaphoreType.DMA
    smem, anywhere = pl.BlockSpec(memory_space=pltpu.SMEM), pl.BlockSpec(memory_space=pl.ANY)
    owned = jax.ShapeDtypeStruct((OWN, 16, D), jnp.float32)
    return pl.pallas_call(
        functools.partial(exchange_kernel, capacity),
        out_shape=(owned, owned, jax.ShapeDtypeStruct((1, SLOTS, 4, D), jnp.bfloat16)),
        in_specs=[smem, smem, anywhere, anywhere, anywhere],
        out_specs=(anywhere, anywhere, anywhere),
        scratch_shapes=[
            vmem((CHUNKS, 2, SLOTS, 4, DC), jnp.bfloat16),
            vmem((CHUNKS, REPLICAS, 16, 4, DC), jnp.bfloat16),
            vmem((CHUNKS, 32, 4, DC), jnp.float32),
            vmem((CHUNKS, 8, OWN, 4, DC), jnp.float32),
            vmem((8, 8, 128), jnp.float32),
            vmem((4, 8, 128), jnp.float32),
            vmem((8, 8, 128), jnp.float32),
            vmem((OWN, 16, D), jnp.float32),
            vmem((OWN, 16, D), jnp.float32),
            vmem((OWN, 16, D), jnp.float32),
            vmem((OWN, 16, D), jnp.float32),
            vmem((CHUNKS, 2, 4, OWN, 4, DC), jnp.float32),
            vmem((CHUNKS, 32, 4, DC), jnp.float32),
            vmem((CHUNKS, 3, capacity, 4, DC), jnp.bfloat16),
            vmem((CHUNKS, 4, capacity, 4, DC), jnp.bfloat16),
            vmem((SLOTS, 4, D), jnp.bfloat16),
        ]
        + [vmem((32, 4, DC), jnp.bfloat16)] * CHUNKS
        + [vmem((4 * capacity, 4, DC), jnp.bfloat16)] * (2 * CHUNKS)
        + [vmem((2, SLOTS, 4, DC), jnp.bfloat16)] * CHUNKS
        + [
            dma((2,)),
            dma((CHUNKS, 2)),
            dma((CHUNKS, 8)),
            dma((CHUNKS, 8)),
            dma((CHUNKS, 8)),
            dma((CHUNKS, 8)),
            dma((17,)),
            dma((17,)),
            dma((CHUNKS, 8)),
            dma((CHUNKS, 8)),
            dma((CHUNKS, 4)),
            dma((CHUNKS, 4)),
            dma((CHUNKS, 4)),
            dma((CHUNKS, 4)),
            dma((CHUNKS, 4)),
            dma((CHUNKS, 4)),
            dma((CHUNKS, 2)),
            dma((CHUNKS, 4)),
        ],
        compiler_params=pltpu.CompilerParams(
            collective_id=capacity, has_side_effects=True, vmem_limit_bytes=56 * 2**20
        ),
        name=f"exchange_{capacity}",
    )(table, coef, deltas, params, momentum)


def tables_kernel(list_ref, hosting_ref, counts_ref, table_ref, coef_ref):
    f32, bf16 = jnp.float32, jnp.bfloat16
    replica = lax.axis_index("replica")

    def iota(shape, axis):
        return lax.broadcasted_iota(jnp.int32, shape, axis)

    def product(left, right, transposed=False):
        return lax.dot_general(
            left.astype(bf16), right.astype(bf16), (((1,), (1 if transposed else 0,)), ((), ())), preferred_element_type=f32
        )

    def as_float(condition):
        return jnp.where(condition, 1.0, 0.0).astype(f32)

    row, col = iota((128, 128), 0), iota((128, 128), 1)
    row8, col8 = iota((8, 128), 0), iota((8, 128), 1)

    def pick_row(array, i):
        return jnp.sum(jnp.where(row8 == i, array, 0.0), axis=0, keepdims=True)

    spread = product(hosting_ref[...].astype(f32), as_float(iota((16, 128), 1) // 8 == iota((16, 128), 0)))
    own_expert = iota((64, 128), 1) % 8 == iota((64, 128), 0) % 8
    hosted = jnp.sum(jnp.where(own_expert, spread, 0.0).reshape(8, 8, 128), axis=1)
    weight = hosted * counts_ref[...].astype(f32)
    totals = jnp.maximum(jnp.sum(weight, axis=0, keepdims=True), 1.0)
    ratio = weight / totals

    entry = iota((8, SLOTS), 1).astype(f32)
    ones_and_entries = jnp.where(iota((8, SLOTS), 0) == 0, 1.0, entry)
    blocks = iota((BLOCKS, SLOTS), 0)

    member = jnp.concatenate(
        [
            product(ones_and_entries, as_float(blocks == list_ref[r : r + 1, :]), transposed=True)[0:1]
            for r in range(REPLICAS)
        ],
        axis=0,
    )
    mine = list_ref[pl.ds(replica, 1), :]
    listed = as_float(blocks == mine)
    entry_of = product(ones_and_entries, listed, transposed=True)[1:2]

    rank = product(member, as_float((row // OWN == col // OWN) & (row < col)))
    coef_ref[0:8, :] = jnp.where(rank < 0.5, ratio, 0.0)
    coef_ref[8:16, :] = jnp.where(rank > 0.5, ratio, 0.0)

    my_rank = pick_row(rank, replica)
    source = entry_of * pick_row(member, replica)
    by_rank = jnp.where((row8 == 0) == (my_rank < 0.5), source, 0.0)
    index = product(by_rank, as_float(row // OWN == col))

    union = jnp.concatenate(
        [jnp.maximum(member[2 * y : 2 * y + 1], member[2 * y + 1 : 2 * y + 2]) for y in range(4)] * 2, axis=0
    )
    place = product(union, as_float((row // 32 == col // 32) & (row < col)))
    my_place = pick_row(place, replica // 2)
    entry_place = product(jnp.broadcast_to(my_place, (8, BLOCKS)), listed)
    most = jnp.max(jnp.where(union > 0.5, place + 1.0, 0.0), keepdims=True)

    table_ref[0:8, :] = index.astype(jnp.int32)
    table_ref[2:3, 0:SLOTS] = jnp.where(mine >= 0, entry_place[0:1].astype(jnp.int32), -1)
    table_ref[3:4, 0:SLOTS] = jnp.maximum(mine, 0) // 32
    table_ref[4:5, :] = jnp.broadcast_to(most.astype(jnp.int32), (1, 128))
    group = jnp.where(col8 // 32 == row8, (col8 % 32).astype(f32), 0.0)
    for y in range(4):
        holds = as_float((place[y : y + 1] == row.astype(f32)) & (union[y : y + 1] > 0.5))
        table_ref[8 + 4 * y : 12 + 4 * y, :] = product(group, holds, transposed=True)[0:4].astype(jnp.int32)


def tables(block_list, hosting, counts):
    return pl.pallas_call(
        tables_kernel,
        out_shape=(jax.ShapeDtypeStruct((24, 128), jnp.int32), jax.ShapeDtypeStruct((16, 128), jnp.float32)),
        name="tables",
    )(block_list, hosting.transpose(0, 2, 1).reshape(64, 16), counts)


def per_device(deltas, block_list, hosting, counts, params, momentum):
    table, coef = tables(block_list, hosting, counts)
    small, full = (functools.partial(exchange, capacity) for capacity in (18, 32))
    return lax.cond(table[4, 0] <= 18, small, full, table, coef, deltas, params, momentum)


def solution(mesh):
    blocks = P("shard", "replica", None)
    entries = P("replica", None, "shard", None)
    return jax.shard_map(
        per_device,
        mesh=mesh,
        in_specs=(entries, P(), P(), P(), blocks, blocks),
        out_specs=(blocks, blocks, entries),
        check_vma=False,
    )
```

```python
import functools
import math

import jax
import jax.numpy as jnp
from jax import lax
from jax.experimental import pallas as pl
from jax.experimental.pallas import tpu as pltpu
from jax.sharding import PartitionSpec as P

D = 6144
ROWS = 128
HALF = D // 2
CHUNKS = 4
EARLY = 1
DC = HALF // CHUNKS
SLOTS = 64
OWN = 4
CAP = 2
REPLICAS = 8
BLOCKS = 128
MESH = pl.DeviceIdType.MESH

decay_rate = 0.9
outer_rate = 0.7
limit_ratio = 0.1


class Place:
    def __init__(self):
        self.replica = lax.axis_index("replica")
        self.shard = lax.axis_index("shard")
        self.y = self.replica // 2
        self.c = self.replica % 2
        self.x = self.shard // 8
        self.z = self.shard % 8
        self.zh = self.z // 4
        self.zl = self.z % 4
        self.self_xy = self.x == self.y
        self.self_z = self.c == self.zh

    def xy_target(self, dx, dc):
        xt = lax.rem(self.x + dx, 4)
        ct = lax.rem(self.c + dc, 2)
        return xt, ct, (2 * self.x + ct, xt * 8 + self.z)

    def xy_source(self, d):
        r = lax.rem(self.replica + d, 8)
        return r, (r, self.y * 8 + self.z)

    def z_target(self, dz):
        zt = lax.rem(self.z + dz, 8)
        return zt, (2 * self.y + self.zh, self.x * 8 + zt)

    def z_source(self, d, dc):
        zs = lax.rem(self.zl + d, 4)
        cs = lax.rem(self.c + dc, 2)
        return zs, cs, (2 * self.y + cs, self.x * 8 + self.c * 4 + zs)

    def shifted(self, dx, dy, dz, dc):
        x = lax.rem(self.x + dx, 4)
        y = lax.rem(self.y + dy, 4)
        z = lax.rem(self.z + dz, 8)
        c = lax.rem(self.c + dc, 2)
        return (y * 2 + c, x * 8 + z)


def columns(half, n):
    return pl.ds(pl.multiple_of(half * HALF + n * DC, 128), DC)


def guarded(maybe_self, condition, act):
    if maybe_self:
        pl.when(jnp.logical_not(condition))(act)
    else:
        act()


def exchange_kernel(
    capacity, table_ref, coef_ref, deltas_ref, params_ref, momentum_ref,
    new_params_ref, new_momentum_ref, host_ref, *scratch,
):
    (
        packed, rx, sums, gx, sq_cx, sq_y, sq_z, params, momentum, new_params, new_momentum,
        kept, base, picked, relay, host,
    ) = scratch[:16]
    blocks = scratch[16 : 16 + CHUNKS]
    near = scratch[16 + CHUNKS : 16 + 2 * CHUNKS]
    far = scratch[16 + 2 * CHUNKS : 16 + 3 * CHUNKS]
    raw = scratch[16 + 3 * CHUNKS : 16 + 4 * CHUNKS]
    (
        load_sem, raw_sem, xy_send, xy_recv, z_send, z_recv, sq_send, sq_recv,
        a_send, a_recv, y_send, y_recv, x_send, x_recv, d_send, d_recv, host_sem, store_sem,
    ) = scratch[16 + 4 * CHUNKS :]
    me = Place()
    sibling = (2 * me.y + 1 - me.c, me.shard)

    def raw_copy(n, half):
        return pltpu.make_async_copy(
            deltas_ref.at[0, :, :, columns(half, n)], raw[n].at[half], raw_sem.at[n, half]
        )

    for n in range(CHUNKS):
        for half in range(2):
            raw_copy(n, half).start()
    load_params = pltpu.make_async_copy(params_ref, params, load_sem.at[0])
    load_momentum = pltpu.make_async_copy(momentum_ref, momentum, load_sem.at[1])
    load_params.start()
    load_momentum.start()

    barrier = pltpu.get_barrier_semaphore()

    def greet(device):
        pl.semaphore_signal(barrier, inc=1, device_id=device, device_id_type=MESH)

    for d in range(8):
        guarded(d == 0, me.self_xy, functools.partial(greet, me.xy_source(d)[1]))
        guarded(d == 0, me.self_z, functools.partial(greet, me.z_target(d)[1]))
    for d in range(4):
        for dc in range(2):
            guarded(d == 0 and dc == 0, me.self_z, functools.partial(greet, me.z_source(d, dc)[2]))
    stages = (
        (sq_cx, 2 * me.x + me.c, [(d, 0, 0, c) for d in (2, 1, 3, 0) for c in (0, 1) if d or c]),
        (sq_y, me.y, [(0, d, 0, 0) for d in (1, 2, 3)]),
        (sq_z, me.z, [(0, 0, d, 0) for d in range(1, 8)]),
    )
    for _, _, offsets in stages:
        for offset in offsets:
            greet(me.shifted(*offset))

    def pack(n):
        for half in range(2):
            raw_copy(n, half).wait()

        def place(owner, carry):
            for k in range(CAP):
                entry = table_ref[k, owner]
                for half in range(2):
                    packed[n, half, owner * CAP + k] = raw[n][half, entry]
            return carry

        lax.fori_loop(0, 32, place, 0)

    pack(0)
    pl.semaphore_wait(
        barrier,
        8 + 16 + 17 - me.self_xy.astype(jnp.int32) - 2 * me.self_z.astype(jnp.int32),
    )

    def xy_copy(n, dx, dc):
        xt, ct, device = me.xy_target(dx, dc)
        return pltpu.make_async_remote_copy(
            src_ref=packed.at[n, ct, pl.ds(xt * 16, 16)],
            dst_ref=rx.at[n, me.replica],
            send_sem=xy_send.at[n, dx * 2 + dc],
            recv_sem=xy_recv.at[n, me.replica],
            device_id=device,
            device_id_type=MESH,
        )

    def xy_arrival(n, d):
        r, device = me.xy_source(d)
        return pltpu.make_async_remote_copy(
            src_ref=packed.at[n, 0, pl.ds(0, 16)],
            dst_ref=rx.at[n, r],
            send_sem=xy_send.at[n, 0],
            recv_sem=xy_recv.at[n, r],
            device_id=device,
            device_id_type=MESH,
        )

    def z_copy(n, dz):
        zt, device = me.z_target(dz)
        return pltpu.make_async_remote_copy(
            src_ref=sums.at[n, pl.ds(zt * 4, 4)],
            dst_ref=gx.at[n, me.zl * 2 + me.c],
            send_sem=z_send.at[n, dz],
            recv_sem=z_recv.at[n, me.zl * 2 + me.c],
            device_id=device,
            device_id_type=MESH,
        )

    def z_arrival(n, d, dc):
        zs, cs, device = me.z_source(d, dc)
        return pltpu.make_async_remote_copy(
            src_ref=sums.at[n, pl.ds(0, 4)],
            dst_ref=gx.at[n, zs * 2 + cs],
            send_sem=z_send.at[n, 0],
            recv_sem=z_recv.at[n, zs * 2 + cs],
            device_id=device,
            device_id_type=MESH,
        )

    xy_order = [(1, 0), (2, 0), (0, 0), (3, 0), (1, 1), (2, 1), (0, 1), (3, 1)]
    z_order = [4, 3, 5, 2, 6, 1, 7, 0]

    def start_z(n):
        for dz in z_order:
            guarded(dz == 0, me.self_z, lambda dz=dz: z_copy(n, dz).start())

    def a_copy(n, d, dc):
        zt, ct, device = me.z_source(d, dc)
        return pltpu.make_async_remote_copy(
            src_ref=kept.at[n, ct, zt],
            dst_ref=base.at[n, pl.ds(me.z * OWN, OWN)],
            send_sem=a_send.at[n, d * 2 + dc],
            recv_sem=a_recv.at[n, me.z],
            device_id=device,
            device_id_type=MESH,
        )

    def a_arrival(n, dz):
        zs, device = me.z_target(dz)
        return pltpu.make_async_remote_copy(
            src_ref=kept.at[n, 0, 0],
            dst_ref=base.at[n, pl.ds(zs * OWN, OWN)],
            send_sem=a_send.at[n, 0],
            recv_sem=a_recv.at[n, zs],
            device_id=device,
            device_id_type=MESH,
        )

    a_order = [(d, dc) for d in (2, 1, 3, 0) for dc in (0, 1)]
    for n in range(CHUNKS):
        if n > 0:
            pack(n)
        for dx, dc in xy_order:
            guarded(dx == 0 and dc == 0, me.self_xy, lambda n=n, dx=dx, dc=dc: xy_copy(n, dx, dc).start())

        @pl.when(me.self_xy)
        def _(n=n):
            def own(k, carry):
                rx[n, me.replica, k] = packed[n, me.c, me.x * 16 + k]
                return carry

            lax.fori_loop(0, 16, own, 0)

        if n == 0:
            load_params.wait()
            load_momentum.wait()
        for half in range(2):
            wide = slice(half * HALF + n * DC, half * HALF + n * DC + DC)
            for pair in range(2):
                rows = slice(pair * 8, pair * 8 + 8)
                for j in range(OWN):
                    keep = params[j, rows, wide] - (outer_rate * decay_rate**2) * momentum[j, rows, wide]
                    kept[n, half, pair * 2, j] = keep[0:4]
                    kept[n, half, pair * 2 + 1, j] = keep[4:8]
        for d, dc in a_order:
            guarded(d == 0 and dc == 0, me.self_z, lambda n=n, d=d, dc=dc: a_copy(n, d, dc).start())

        @pl.when(me.self_z)
        def _(n=n):
            for j in range(OWN):
                base[n, me.z * OWN + j] = kept[n, me.c, me.zl, j]

    total = jnp.zeros((4, DC), jnp.float32)
    for n in range(CHUNKS):
        for d in range(8):
            guarded(d == 0, me.self_xy, lambda n=n, d=d: xy_arrival(n, d).wait_recv())

        def mix(owner, total, n=n):
            acc = [jnp.zeros((4, DC), jnp.float32) for _ in range(OWN)]
            for r in range(REPLICAS):
                for k in range(CAP):
                    rows = rx[n, r, owner * CAP + k].astype(jnp.float32)
                    for j in range(OWN):
                        acc[j] = acc[j] + coef_ref[k * REPLICAS + r, me.x * 32 + owner * OWN + j] * rows
            for j in range(OWN):
                sums[n, owner * OWN + j] = acc[j]
                total = total + acc[j] * acc[j]
            return total

        total = lax.fori_loop(0, 8, mix, total)
        if n < EARLY:
            start_z(n)

        @pl.when(me.self_z)
        def _(n=n):
            for j in range(OWN):
                gx[n, me.zl * 2 + me.c, j] = sums[n, me.z * OWN + j]

    value = jnp.full((8, 128), jnp.sum(total), jnp.float32)
    first = 0
    for slots, mine, offsets in stages:
        slots[mine] = value
        copies = []
        for i, offset in enumerate(offsets):
            copy = pltpu.make_async_remote_copy(
                src_ref=slots.at[mine],
                dst_ref=slots.at[mine],
                send_sem=sq_send.at[first + i],
                recv_sem=sq_recv.at[first + i],
                device_id=me.shifted(*offset),
                device_id_type=MESH,
            )
            copy.start()
            copies.append(copy)
        if slots is sq_z:
            for n in range(EARLY, CHUNKS):
                start_z(n)
        for copy in copies:
            copy.wait()
        value = slots[0]
        for i in range(1, slots.shape[0]):
            value = value + slots[i]
        first += len(offsets)

    limit = limit_ratio * math.sqrt(BLOCKS * ROWS * D)
    factor = jnp.minimum(1.0, limit / jnp.sqrt(value + 1e-06))[0:1, 0:1]
    step_size = (outer_rate * (1.0 + decay_rate)) * factor

    def store_copies(n):
        copies = []
        for half in range(2):
            wide = slice(half * HALF + n * DC, half * HALF + n * DC + DC)
            for i, (inside, outside) in enumerate(
                ((new_params, new_params_ref), (new_momentum, new_momentum_ref))
            ):
                copies.append(
                    pltpu.make_async_copy(
                        inside.at[:, :, wide], outside.at[:, :, wide], store_sem.at[n, half * 2 + i]
                    )
                )
        return copies

    def update(n):
        for d in range(4):
            for dc in range(2):
                guarded(d == 0 and dc == 0, me.self_z, lambda d=d, dc=dc: z_arrival(n, d, dc).wait_recv())
        for half in range(2):
            wide = slice(half * HALF + n * DC, half * HALF + n * DC + DC)
            for pair in range(2):
                rows = slice(pair * 8, pair * 8 + 8)
                for j in range(OWN):
                    grad = jnp.concatenate([gx[n, pair * 4 + half, j], gx[n, pair * 4 + 2 + half, j]], axis=0)
                    scaled = factor * grad
                    moved = decay_rate * momentum[j, rows, wide] + scaled
                    new_momentum[j, rows, wide] = moved
                    new_params[j, rows, wide] = params[j, rows, wide] - outer_rate * (scaled + decay_rate * moved)
        for copy in store_copies(n):
            copy.start()

    def y_copy(n, d, arrival=False):
        ys = lax.rem(me.y + d, 4) if arrival else me.y
        return pltpu.make_async_remote_copy(
            src_ref=picked.at[n, d - 1],
            dst_ref=relay.at[n, ys],
            send_sem=y_send.at[n, d],
            recv_sem=y_recv.at[n, ys],
            device_id=me.shifted(0, d, 0, 0),
            device_id_type=MESH,
        )

    def x_copy(n, d, arrival=False):
        xs = lax.rem(me.x + d, 4)
        xd = xs if arrival else me.x
        return pltpu.make_async_remote_copy(
            src_ref=relay.at[n, xs],
            dst_ref=near[n].at[pl.ds(xd * capacity, capacity)],
            send_sem=x_send.at[n, d],
            recv_sem=x_recv.at[n, xd],
            device_id=me.shifted(d, 0, 0, 0),
            device_id_type=MESH,
        )

    def d_copy(n, d):
        xs = lax.rem(me.x + d, 4)
        return pltpu.make_async_remote_copy(
            src_ref=near[n].at[pl.ds(xs * capacity, capacity)],
            dst_ref=far[n].at[pl.ds(xs * capacity, capacity)],
            send_sem=d_send.at[n, xs],
            recv_sem=d_recv.at[n, xs],
            device_id=sibling,
            device_id_type=MESH,
        )

    def host_copy(n, half):
        return pltpu.make_async_copy(
            host.at[:, :, columns(half, n)], host_ref.at[0, :, :, columns(half, n)], host_sem.at[n, half]
        )

    order = (2, 1, 3)

    def start_y(n):
        for dz in range(8):
            guarded(dz == 0, me.self_z, lambda dz=dz: a_arrival(n, dz).wait_recv())

        def fresh(block, carry):
            blocks[n][block] = (base[n, block] - step_size * sums[n, block]).astype(jnp.bfloat16)
            return carry

        lax.fori_loop(0, 32, fresh, 0)

        def pick(k, carry):
            for d in range(1, 4):
                picked[n, d - 1, k] = blocks[n][table_ref[8 + lax.rem(me.y + d, 4) * 4 + me.x, k]]
            relay[n, me.y, k] = blocks[n][table_ref[8 + me.y * 4 + me.x, k]]
            return carry

        lax.fori_loop(0, capacity, pick, 0)
        for d in order:
            y_copy(n, d).start()

    def start_x(n):
        for d in order:
            y_copy(n, d, arrival=True).wait_recv()
        for d in order:
            x_copy(n, d).start()

        def own(k, carry):
            near[n][me.x * capacity + k] = relay[n, me.x, k]
            return carry

        lax.fori_loop(0, capacity, own, 0)

    def start_d(n):
        d_copy(n, 0).start()
        for d in order:
            x_copy(n, d, arrival=True).wait_recv()
            d_copy(n, d).start()

    def unpack(n):
        for d in range(4):
            d_copy(n, d).wait_recv()

        def entry(k, carry):
            place = table_ref[2, k]
            safe = table_ref[3, k] * capacity + jnp.maximum(place, 0)
            for rows, half in ((near[n], me.c), (far[n], 1 - me.c)):
                value = rows[safe]
                host[k, :, columns(half, n)] = jnp.where(place >= 0, value, jnp.zeros_like(value))
            return carry

        lax.fori_loop(0, SLOTS, entry, 0)
        for half in range(2):
            host_copy(n, half).start()

    for step in range(CHUNKS + 6):
        for lag, stage in ((0, start_y), (2, start_x), (4, start_d), (5, unpack), (6, update)):
            if 0 <= step - lag < CHUNKS:
                stage(step - lag)

    for n in range(CHUNKS):
        for dx, dc in xy_order:
            guarded(dx == 0 and dc == 0, me.self_xy, lambda n=n, dx=dx, dc=dc: xy_copy(n, dx, dc).wait_send())
        for dz in z_order:
            guarded(dz == 0, me.self_z, lambda n=n, dz=dz: z_copy(n, dz).wait_send())
        for d, dc in a_order:
            guarded(d == 0 and dc == 0, me.self_z, lambda n=n, d=d, dc=dc: a_copy(n, d, dc).wait_send())
        for d in order:
            y_copy(n, d).wait_send()
            x_copy(n, d).wait_send()
        for d in range(4):
            d_copy(n, d).wait_send()
    for n in range(CHUNKS):
        for copy in store_copies(n):
            copy.wait()
        for half in range(2):
            host_copy(n, half).wait()


def exchange(capacity, table, coef, deltas, params, momentum):
    vmem, dma = pltpu.VMEM, pltpu.SemaphoreType.DMA
    smem, anywhere = pl.BlockSpec(memory_space=pltpu.SMEM), pl.BlockSpec(memory_space=pl.ANY)
    owned = jax.ShapeDtypeStruct((OWN, 16, D), jnp.float32)
    return pl.pallas_call(
        functools.partial(exchange_kernel, capacity),
        out_shape=(owned, owned, jax.ShapeDtypeStruct((1, SLOTS, 4, D), jnp.bfloat16)),
        in_specs=[smem, smem, anywhere, anywhere, anywhere],
        out_specs=(anywhere, anywhere, anywhere),
        scratch_shapes=[
            vmem((CHUNKS, 2, SLOTS, 4, DC), jnp.bfloat16),
            vmem((CHUNKS, REPLICAS, 16, 4, DC), jnp.bfloat16),
            vmem((CHUNKS, 32, 4, DC), jnp.float32),
            vmem((CHUNKS, 8, OWN, 4, DC), jnp.float32),
            vmem((8, 8, 128), jnp.float32),
            vmem((4, 8, 128), jnp.float32),
            vmem((8, 8, 128), jnp.float32),
            vmem((OWN, 16, D), jnp.float32),
            vmem((OWN, 16, D), jnp.float32),
            vmem((OWN, 16, D), jnp.float32),
            vmem((OWN, 16, D), jnp.float32),
            vmem((CHUNKS, 2, 4, OWN, 4, DC), jnp.float32),
            vmem((CHUNKS, 32, 4, DC), jnp.float32),
            vmem((CHUNKS, 3, capacity, 4, DC), jnp.bfloat16),
            vmem((CHUNKS, 4, capacity, 4, DC), jnp.bfloat16),
            vmem((SLOTS, 4, D), jnp.bfloat16),
        ]
        + [vmem((32, 4, DC), jnp.bfloat16)] * CHUNKS
        + [vmem((4 * capacity, 4, DC), jnp.bfloat16)] * (2 * CHUNKS)
        + [vmem((2, SLOTS, 4, DC), jnp.bfloat16)] * CHUNKS
        + [
            dma((2,)),
            dma((CHUNKS, 2)),
            dma((CHUNKS, 8)),
            dma((CHUNKS, 8)),
            dma((CHUNKS, 8)),
            dma((CHUNKS, 8)),
            dma((17,)),
            dma((17,)),
            dma((CHUNKS, 8)),
            dma((CHUNKS, 8)),
            dma((CHUNKS, 4)),
            dma((CHUNKS, 4)),
            dma((CHUNKS, 4)),
            dma((CHUNKS, 4)),
            dma((CHUNKS, 4)),
            dma((CHUNKS, 4)),
            dma((CHUNKS, 2)),
            dma((CHUNKS, 4)),
        ],
        compiler_params=pltpu.CompilerParams(
            collective_id=capacity, has_side_effects=True, vmem_limit_bytes=56 * 2**20
        ),
        name=f"exchange_{capacity}",
    )(table, coef, deltas, params, momentum)


def tables_kernel(list_ref, hosting_ref, counts_ref, table_ref, coef_ref):
    f32, bf16 = jnp.float32, jnp.bfloat16
    replica = lax.axis_index("replica")

    def iota(shape, axis):
        return lax.broadcasted_iota(jnp.int32, shape, axis)

    def product(left, right, transposed=False):
        return lax.dot_general(
            left.astype(bf16), right.astype(bf16), (((1,), (1 if transposed else 0,)), ((), ())), preferred_element_type=f32
        )

    def as_float(condition):
        return jnp.where(condition, 1.0, 0.0).astype(f32)

    row, col = iota((128, 128), 0), iota((128, 128), 1)
    row8, col8 = iota((8, 128), 0), iota((8, 128), 1)

    def pick_row(array, i):
        return jnp.sum(jnp.where(row8 == i, array, 0.0), axis=0, keepdims=True)

    spread = product(hosting_ref[...].astype(f32), as_float(iota((16, 128), 1) // 8 == iota((16, 128), 0)))
    own_expert = iota((64, 128), 1) % 8 == iota((64, 128), 0) % 8
    hosted = jnp.sum(jnp.where(own_expert, spread, 0.0).reshape(8, 8, 128), axis=1)
    weight = hosted * counts_ref[...].astype(f32)
    totals = jnp.maximum(jnp.sum(weight, axis=0, keepdims=True), 1.0)
    ratio = weight / totals

    entry = iota((8, SLOTS), 1).astype(f32)
    ones_and_entries = jnp.where(iota((8, SLOTS), 0) == 0, 1.0, entry)
    blocks = iota((BLOCKS, SLOTS), 0)

    member = jnp.concatenate(
        [
            product(ones_and_entries, as_float(blocks == list_ref[r : r + 1, :]), transposed=True)[0:1]
            for r in range(REPLICAS)
        ],
        axis=0,
    )
    mine = list_ref[pl.ds(replica, 1), :]
    listed = as_float(blocks == mine)
    entry_of = product(ones_and_entries, listed, transposed=True)[1:2]

    rank = product(member, as_float((row // OWN == col // OWN) & (row < col)))
    coef_ref[0:8, :] = jnp.where(rank < 0.5, ratio, 0.0)
    coef_ref[8:16, :] = jnp.where(rank > 0.5, ratio, 0.0)

    my_rank = pick_row(rank, replica)
    source = entry_of * pick_row(member, replica)
    by_rank = jnp.where((row8 == 0) == (my_rank < 0.5), source, 0.0)
    index = product(by_rank, as_float(row // OWN == col))

    union = jnp.concatenate(
        [jnp.maximum(member[2 * y : 2 * y + 1], member[2 * y + 1 : 2 * y + 2]) for y in range(4)] * 2, axis=0
    )
    place = product(union, as_float((row // 32 == col // 32) & (row < col)))
    my_place = pick_row(place, replica // 2)
    entry_place = product(jnp.broadcast_to(my_place, (8, BLOCKS)), listed)
    most = jnp.max(jnp.where(union > 0.5, place + 1.0, 0.0), keepdims=True)

    table_ref[0:8, :] = index.astype(jnp.int32)
    table_ref[2:3, 0:SLOTS] = jnp.where(mine >= 0, entry_place[0:1].astype(jnp.int32), -1)
    table_ref[3:4, 0:SLOTS] = jnp.maximum(mine, 0) // 32
    table_ref[4:5, :] = jnp.broadcast_to(most.astype(jnp.int32), (1, 128))
    group = jnp.where(col8 // 32 == row8, (col8 % 32).astype(f32), 0.0)
    for y in range(4):
        holds = as_float((place[y : y + 1] == row.astype(f32)) & (union[y : y + 1] > 0.5))
        table_ref[8 + 4 * y : 12 + 4 * y, :] = product(group, holds, transposed=True)[0:4].astype(jnp.int32)


def tables(block_list, hosting, counts):
    return pl.pallas_call(
        tables_kernel,
        out_shape=(jax.ShapeDtypeStruct((24, 128), jnp.int32), jax.ShapeDtypeStruct((16, 128), jnp.float32)),
        name="tables",
    )(block_list, hosting.transpose(0, 2, 1).reshape(64, 16), counts)


def per_device(deltas, block_list, hosting, counts, params, momentum):
    table, coef = tables(block_list, hosting, counts)
    small, full = (functools.partial(exchange, capacity) for capacity in (18, 32))
    return lax.cond(table[4, 0] <= 18, small, full, table, coef, deltas, params, momentum)


def solution(mesh):
    blocks = P("shard", "replica", None)
    entries = P("replica", None, "shard", None)
    return jax.shard_map(
        per_device,
        mesh=mesh,
        in_specs=(entries, P(), P(), P(), blocks, blocks),
        out_specs=(blocks, blocks, entries),
        check_vma=False,
    )
```
